32 devices in a mesh: seq: 16 (over z, y, core), grp: 2 (over x).
Axes of the slice: x: 2, y: 2, z: 4, core: 2. Of those that a mesh axis runs over, the one named last changes fastest.
Arguments:
- queries: bfloat16 [4096, 3584], P(('grp', 'seq')), parts along dimension 0, may hold values from -5 to 5
- keys: bfloat16 [4096, 512], P(('grp', 'seq')), parts along dimension 0, may hold values from -5 to 5
- values: bfloat16 [4096, 512], P(('grp', 'seq')), parts along dimension 0, may hold values from -6 to 6
- doc_lengths: int32 [16], P('grp'), parts along dimension 0, may hold values from 1 to 1280, 2048 in all
Outputs:
- attended: bfloat16 [4096, 3584], P(('grp', 'seq')), parts along dimension 0
The draws below stay inside these ranges and needn't reach their ends.
There are 2 independent parts, one for each index of `grp`. The reference program is written for one: setup_inputs(seed, part) draws one part's arguments, and reference() takes and returns one part's arrays. A program takes and returns all parts, laid end to end along the dimension named above; each array names one. Nothing has to cross between parts.
Inputs may be any that keep to these rules, and one draw needn't show every extreme that they name: `doc_lengths`: the 8 documents lie one after another and their lengths sum to 2048; the longest has exactly 1280 tokens.
All inputs are finite; a program needn't handle non-finite values.
Results may differ from the reference program's by a relative error of at most 0.0085.
Values may be sent and summed in bfloat16 or wider, within the bound.
No kernel may reach another device: no remote copies, remote signals or barrier semaphores. Data moves between devices by JAX's collectives and lax.ppermute only.
A program may use at most 192 MiB of HBM per device.

```python
import math
import jax
import jax.numpy as jnp
import numpy as np
from jax import lax

HEADS = 28
KV_HEADS = 4
HEAD_DIM = 128
DOCS = 8
SEQ_LEN = 2048
MOST_DOC = 1280


def draw_keys(key, part):
    base_key = jax.random.fold_in(key, 21)
    base_draw = jnp.clip(jax.random.normal(base_key, (SEQ_LEN, KV_HEADS, HEAD_DIM), jnp.float32), -5.0, 5.0)
    return base_draw.reshape(SEQ_LEN, KV_HEADS * HEAD_DIM).astype(jnp.bfloat16)


def draw_queries(key, part):
    base_key = jax.random.fold_in(key, 31)
    group_size = HEADS // KV_HEADS
    shape_full = (SEQ_LEN, KV_HEADS, group_size, HEAD_DIM)
    base_draw = jnp.clip(1.5 * jax.random.normal(base_key, shape_full, jnp.float32), -5.0, 5.0)
    return base_draw.reshape(SEQ_LEN, HEADS * HEAD_DIM).astype(jnp.bfloat16)


def level_of(own_key, dims, pieces, low, high):
    factor_of = 1.0
    for axis_at, parts in pieces:
        draws = jax.random.uniform(jax.random.fold_in(jax.random.fold_in(own_key, 6), axis_at), (parts,), jnp.float32, low / len(pieces), high / len(pieces))
        factor_of = factor_of * jnp.repeat(jnp.exp(draws), dims[axis_at] // parts).reshape((-1,) + (1,) * (len(dims) - 1 - axis_at))
    return factor_of


def length_profile(amount, total, most, lean):
    portions = [(1 << 20) // math.isqrt(grade ** lean) + 1 for grade in range(2, amount + 1)]
    spare, counts = total - most - (amount - 1), [1] * (amount - 1)
    while spare > 0:
        movable = [i for i in range(amount - 1) if counts[i] < most]
        whole, remaining = sum([portions[i] for i in movable]), spare
        for i in movable:
            addition = min(most - counts[i], max(1, remaining * portions[i] // whole), spare)
            counts[i] = counts[i] + addition
            spare = spare - addition
    return np.array([most] + counts)


def uneven_parts(own_key, number_of, total, limit, slope):
    if number_of == 2:
        one = jax.random.randint(own_key, (), max(1, total - limit), min(limit, total - 1) + 1)
        return jnp.stack([one, total - one])
    sizes = jnp.asarray(length_profile(number_of, total, limit, slope), jnp.int32)
    pairs = (number_of - 1) // 2
    donor, receiver = sizes[1:1 + 2 * pairs:2], sizes[2:2 + 2 * pairs:2]
    margin = jnp.minimum(donor - 1, limit - receiver)
    moved = jax.random.randint(jax.random.fold_in(own_key, 1), (pairs,), 0, 1 << 20) % (margin + 1)
    sizes = sizes.at[1:1 + 2 * pairs:2].set(donor - moved).at[2:2 + 2 * pairs:2].set(receiver + moved)
    return sizes[jax.random.permutation(jax.random.fold_in(own_key, 2), number_of)]


def noise(own_key, extent, deviation, most, pieces=(), kind=jnp.bfloat16):
    gain = level_of(own_key, extent, pieces, -0.22, 0.18) if pieces else 1.0
    values = jax.random.normal(own_key, extent, jnp.float32) * deviation * gain
    return jnp.minimum(jnp.maximum(values, -most), most).astype(kind)


def setup_inputs(seed: int = 0, part: int = 0) -> dict:
    key_list = jax.random.split(jax.random.key(seed), 5)
    part_keys = jax.random.split(jax.random.fold_in(key_list[4], part), 5)
    queries = draw_queries(jax.random.fold_in(jax.random.fold_in(key_list[4], part), 71), part)
    keys = draw_keys(jax.random.fold_in(jax.random.fold_in(key_list[4], part), 71), part)
    values = noise(part_keys[2], (SEQ_LEN, KV_HEADS * HEAD_DIM), 1.0, 6.0, ((0, 16),))
    doc_lengths = uneven_parts(part_keys[3], DOCS, SEQ_LEN, MOST_DOC, 1).astype(jnp.int32)
    return {"queries": queries, "keys": keys, "values": values, "doc_lengths": doc_lengths}


rope_base = 1000000.0
negative = -1.0e30


def doc_place(position, doc_lengths):
    doc_ends = jnp.cumsum(doc_lengths).astype(jnp.int32)
    beyond = position[:, None] >= doc_ends[None, :]
    doc_index = jnp.sum(beyond.astype(jnp.int32), axis=1).astype(jnp.int32)
    doc_start = jnp.sum(jnp.where(beyond, doc_lengths[None, :], 0), axis=1).astype(jnp.int32)
    return doc_index, doc_start


def rotate(values_in, within_doc, head_count):
    row_count = values_in.shape[0]
    half_dim = HEAD_DIM // 2
    inverse_freq = jnp.power(jnp.float32(rope_base), -2.0 * jnp.arange(half_dim, dtype=jnp.float32) / HEAD_DIM)
    angles = within_doc.astype(jnp.float32)[:, None] * inverse_freq[None, :]
    cosine = jnp.cos(angles)[:, None, :]
    sines = jnp.sin(angles)[:, None, :]
    fields = values_in.astype(jnp.float32).reshape(row_count, head_count, HEAD_DIM)
    lower_half = fields[..., :half_dim]
    upper_half = fields[..., half_dim:]
    rotated = jnp.concatenate([lower_half * cosine - upper_half * sines, upper_half * cosine + lower_half * sines], axis=-1)
    return rotated.reshape(row_count, head_count * HEAD_DIM).astype(jnp.bfloat16)


def reference(queries, keys, values, doc_lengths):
    seq_total = queries.shape[0]
    group_size = HEADS // KV_HEADS
    score_scale = HEAD_DIM ** -0.5
    position = jnp.arange(seq_total, dtype=jnp.int32)
    doc_index, doc_start = doc_place(position, doc_lengths)
    within_doc = position - doc_start
    q_rot = rotate(queries, within_doc, HEADS)
    k_rot = rotate(keys, within_doc, KV_HEADS)
    k_heads = k_rot.reshape(seq_total, KV_HEADS, HEAD_DIM).astype(jnp.float32)
    v_heads = values.reshape(seq_total, KV_HEADS, HEAD_DIM).astype(jnp.float32)
    block_rows = min(512, seq_total)
    q_blocks = q_rot.reshape(seq_total // block_rows, block_rows, KV_HEADS, group_size, HEAD_DIM)
    pos_blocks = position.reshape(-1, block_rows)
    doc_blocks = doc_index.reshape(-1, block_rows)

    def attend_block(packed_in):
        q_block, pos_block, doc_block = packed_in
        scores = jnp.einsum("qkgd,skd->qkgs", q_block.astype(jnp.float32), k_heads) * score_scale
        allowed = (doc_index[None, :] == doc_block[:, None]) & (position[None, :] <= pos_block[:, None])
        allowed = allowed[:, None, None, :]
        scores = jnp.where(allowed, scores, negative)
        row_max = jnp.max(scores, axis=-1, keepdims=True)
        weight = jnp.where(allowed, jnp.exp(scores - row_max), 0.0)
        weight_sum = jnp.sum(weight, axis=-1)
        weight_b = lax.optimization_barrier(weight.astype(jnp.bfloat16))
        mixed_out = jnp.einsum("qkgs,skd->qkgd", weight_b.astype(jnp.float32), v_heads)
        mixed_out = mixed_out / weight_sum[..., None]
        return mixed_out.reshape(block_rows, HEADS * HEAD_DIM).astype(jnp.bfloat16)

    attended = lax.map(attend_block, (q_blocks, pos_blocks, doc_blocks))
    return attended.reshape(seq_total, HEADS * HEAD_DIM)
```

```python
import functools

import jax
import jax.numpy as jnp
import numpy as np
from jax import lax
from jax.experimental import pallas as pl
from jax.experimental.pallas import tpu as pltpu
from jax.sharding import PartitionSpec as P

HEADS = 28
KV_HEADS = 4
HEAD_DIM = 128
GROUP = HEADS // KV_HEADS
ROPE_BASE = 1000000.0
NEGATIVE = -1e30
SCORE_SCALE = HEAD_DIM ** (-0.5) * 1.4426950408889634
NOWHERE = 1 << 28
VMEM_LIMIT = 24 * 1024 * 1024


def cycles(wanted, count):
    pairs = dict(wanted)
    starts = [s for s in pairs if s not in set(pairs.values())]
    for start in starts:
        at = start
        while at in pairs:
            at = pairs[at]
        pairs[at] = start
    for i in range(count):
        pairs.setdefault(i, i)
    assert sorted(pairs.values()) == list(range(count))
    return sorted(pairs.items())


class Piece:
    def __init__(self, data, source):
        self.data, self.source = data, source

    def move(self, pairs):
        source = list(self.source)
        for s, t in pairs:
            source[t] = self.source[s]
        return Piece(lax.ppermute(self.data, "seq", pairs), source)


def rotated(x, cosine, sine):
    return x * cosine + pltpu.roll(x, HEAD_DIM // 2, 1) * sine


def prepare_kernel(k_ref, v_ref, cos_ref, sin_ref, kv_ref):
    width = KV_HEADS * HEAD_DIM
    cosine, sine = cos_ref[...], sin_ref[...]
    for g in range(KV_HEADS):
        cols = slice(g * HEAD_DIM, (g + 1) * HEAD_DIM)
        kv_ref[:, cols] = rotated(k_ref[:, cols].astype(jnp.float32), cosine, sine).astype(jnp.bfloat16)
    kv_ref[:, width:] = v_ref[...]


def prepare(keys, values, cosine, sine):
    rows = keys.shape[0]
    return pl.pallas_call(
        prepare_kernel,
        out_shape=jax.ShapeDtypeStruct((rows, 2 * KV_HEADS * HEAD_DIM), jnp.bfloat16),
        cost_estimate=pl.CostEstimate(flops=10**6, bytes_accessed=6 * 10**5, transcendentals=0),
        compiler_params=pltpu.CompilerParams(vmem_limit_bytes=VMEM_LIMIT),
        name="prepare",
    )(keys, values, cosine, sine)


def attend_kernel(count, first, last, *refs):
    refs = list(refs)
    take = lambda n: [refs.pop(0) for _ in range(n)]
    lengths_ref, bases_ref = take(2)
    if first:
        cos_ref, sin_ref = take(2)
    (q_ref,) = take(1)
    k_refs, v_refs = take(count), take(count)
    if not first:
        max_in, sum_in, acc_in = take(3)
    if last:
        (out_ref,) = take(1)
    else:
        if first:
            (q_out,) = take(1)
        max_out, sum_out, acc_out = take(3)
    (bias_ref,) = take(1)

    me = lax.axis_index("seq")
    rows = k_refs[0].shape[0]

    @pl.when(pl.program_id(0) == 0)
    def _():
        own = me * rows + lax.broadcasted_iota(jnp.int32, (rows, rows), 0)
        start = jnp.zeros((rows, rows), jnp.int32)
        end = 0
        for d in range(lengths_ref.shape[0]):
            end = end + lengths_ref[d]
            start = start + jnp.where(own >= end, lengths_ref[d], 0)
        for b in range(count):
            place = bases_ref[b, me] + lax.broadcasted_iota(jnp.int32, (rows, rows), 1)
            allowed = (place >= start) & (place <= own)
            bias_ref[:, b * rows:(b + 1) * rows] = jnp.where(allowed, 0.0, NEGATIVE)

    if first:
        parts = []
        for h in range(GROUP):
            head = q_ref[:, h * HEAD_DIM:(h + 1) * HEAD_DIM].astype(jnp.float32)
            parts.append((rotated(head, cos_ref[...], sin_ref[...]) * SCORE_SCALE).astype(jnp.bfloat16))
        q = jnp.concatenate(parts, axis=0)
        q_out[0] = q
    else:
        q = q_ref[0]
    k = jnp.concatenate([r[...] for r in k_refs], axis=0)
    v = jnp.concatenate([r[...] for r in v_refs], axis=0)
    scores = lax.dot_general(q, k, (((1,), (1,)), ((), ())), preferred_element_type=jnp.float32)
    scores = scores.reshape(GROUP, rows, count * rows) + bias_ref[...][None]
    scores = scores.reshape(GROUP * rows, count * rows)
    top = jnp.max(scores, axis=1, keepdims=True)
    if not first:
        top = jnp.maximum(max_in[0][:, :1], top)
    weight = jnp.exp2(scores - top)
    part = weight[:, :HEAD_DIM]
    for c in range(HEAD_DIM, count * rows, HEAD_DIM):
        part = part + weight[:, c:c + HEAD_DIM]
    acc = jnp.dot(weight.astype(jnp.bfloat16), v, preferred_element_type=jnp.float32)
    if not first:
        shrink = jnp.exp2(max_in[0] - top)
        acc = acc + acc_in[0] * shrink
        part = part + sum_in[0] * shrink
    if last:
        acc = acc / jnp.sum(part, axis=1, keepdims=True)
        for h in range(GROUP):
            out_ref[:, h * HEAD_DIM:(h + 1) * HEAD_DIM] = acc[h * rows:(h + 1) * rows].astype(jnp.bfloat16)
    else:
        max_out[0] = jnp.broadcast_to(top, acc.shape)
        sum_out[0] = part
        acc_out[0] = acc


def attend(lengths, q, pieces, tables, state=None, turn=None, last=False):
    first = state is None
    count = len(pieces)
    rows = pieces[0].data.shape[0]
    stacked = (KV_HEADS, GROUP * rows, HEAD_DIM)
    smem = pl.BlockSpec(memory_space=pltpu.SMEM)
    whole = pl.BlockSpec((rows, HEAD_DIM), lambda g: (0, 0))
    wide = pl.BlockSpec((rows, GROUP * HEAD_DIM), lambda g: (0, g))
    deep = pl.BlockSpec((1, GROUP * rows, HEAD_DIM), lambda g: (g, 0, 0))
    key_spec = pl.BlockSpec((rows, HEAD_DIM), lambda g: (0, g))
    value_spec = pl.BlockSpec((rows, HEAD_DIM), lambda g: (0, KV_HEADS + g))
    data = [p.data for p in pieces]
    args = [lengths, tables]
    specs = [smem, smem]
    if first:
        args += list(turn)
        specs += [whole] * 2
    args += [q] + data + data
    specs += [wide if first else deep] + [key_spec] * count + [value_spec] * count
    state_shape = [jax.ShapeDtypeStruct(stacked, jnp.float32)] * 3
    aliases = {}
    if not first:
        if not last:
            aliases = {len(args) + n: n for n in range(3)}
        args += list(state)
        specs += [deep] * 3
    if last:
        out_shape = jax.ShapeDtypeStruct((rows, HEADS * HEAD_DIM), jnp.bfloat16)
        out_specs = wide
    elif first:
        out_shape = [jax.ShapeDtypeStruct(stacked, jnp.bfloat16)] + state_shape
        out_specs = [deep] * 4
    else:
        out_shape = state_shape
        out_specs = [deep] * 3
    flops = 4 * rows * HEADS * count * rows * HEAD_DIM
    return pl.pallas_call(
        functools.partial(attend_kernel, count, first, last),
        out_shape=out_shape,
        grid=(KV_HEADS,),
        in_specs=specs,
        out_specs=out_specs,
        scratch_shapes=[pltpu.VMEM((rows, count * rows), jnp.float32)],
        input_output_aliases=aliases,
        cost_estimate=pl.CostEstimate(
            flops=flops, bytes_accessed=10**7, transcendentals=rows * HEADS * count * rows
        ),
        compiler_params=pltpu.CompilerParams(vmem_limit_bytes=VMEM_LIMIT),
        name="attend%d%s" % (count, "f" if first else "l" if last else "m"),
    )(*args)


def per_device(count, queries, keys, values, doc_lengths):
    rows = queries.shape[0]
    tokens = rows * count
    most_doc = tokens * 5 // 8
    reach = -(-(most_doc - 1) // rows)
    chip_reach = -(-(most_doc - 1) // (2 * rows))

    half = HEAD_DIM // 2
    place = lax.axis_index("seq") * rows + jnp.arange(rows, dtype=jnp.int32)
    freq = jnp.power(jnp.float32(ROPE_BASE), -2.0 * jnp.arange(half, dtype=jnp.float32) / HEAD_DIM)
    angle = place.astype(jnp.float32)[:, None] * freq[None, :]
    cosine, sine = jnp.cos(angle), jnp.sin(angle)
    cosine = jnp.concatenate([cosine, cosine], axis=1)
    sine = jnp.concatenate([-sine, sine], axis=1)

    def closed(shift, keep):
        return cycles({i: i + shift for i in range(count) if i + shift < count and keep(i)}, count)

    sibling = [(i, i ^ 1) for i in range(count)]
    across = [(i, i ^ 2) for i in range(count)]
    own = Piece(prepare(keys, values, cosine, sine), list(range(count)))
    stages = [[own.move(sibling)]]
    a, before = own, None
    for s in range(1, chip_reach // 2 + 1):
        b = a.move(across)
        a = a.move(closed(4, lambda i: i >= 4 * (s - 1)))
        stages.append([a, b, a.move(sibling), b.move(sibling)])
        before = b
    if chip_reach % 2:
        near = 4 * (chip_reach // 2)
        c = before.move(closed(4, lambda i: not i & 2 and i >= 4 * (chip_reach // 2 - 1)))
        a = a.move(closed(2, lambda i: i >= near))
        stages.append([a, c, a.move(sibling), c.move(sibling)])
    else:
        b = a.move(across)
        stages.append([b, b.move(sibling)])

    seen = [{i} for i in range(count)]
    tables = []
    for n, pieces in enumerate(stages):
        pieces = ([own] if n == 0 else []) + pieces
        table = np.full((len(pieces), count), NOWHERE, np.int32)
        for b, piece in enumerate(pieces):
            for i in range(count):
                j = piece.source[i]
                if piece is own or (i - reach <= j < i and j not in seen[i]):
                    seen[i].add(j)
                    table[b, i] = j * rows
        stages[n] = pieces
        tables.append(jnp.asarray(table))
    for i in range(count):
        assert seen[i] == set(range(max(0, i - reach), i + 1))

    q, *state = attend(doc_lengths, queries, stages[0], tables[0], turn=(cosine, sine))
    for n in range(1, len(stages) - 1):
        state = attend(doc_lengths, q, stages[n], tables[n], state=state)
    return attend(doc_lengths, q, stages[-1], tables[-1], state=state, last=True)


def solution(mesh):
    return jax.shard_map(
        functools.partial(per_device, mesh.shape["seq"]),
        mesh=mesh,
        in_specs=(
            P(("grp", "seq"), None),
            P(("grp", "seq"), None),
            P(("grp", "seq"), None),
            P("grp"),
        ),
        out_specs=P(("grp", "seq"), None),
        check_vma=False,
    )
```

```python
import functools

import jax
import jax.numpy as jnp
import numpy as np
from jax import lax
from jax.experimental import pallas as pl
from jax.experimental.pallas import tpu as pltpu
from jax.sharding import PartitionSpec as P


HEADS = 28
KV_HEADS = 4
HEAD_DIM = 128
GROUP = HEADS // KV_HEADS
ROPE_BASE = 1000000.0
SCORE_SCALE = HEAD_DIM ** (-0.5) * 1.4426950408889634
MASKED = -65536.0
NOWHERE = 1 << 28
VMEM_LIMIT = 24 * 1024 * 1024
SLAB = 32


def cycles(wanted, count):
    pairs = dict(wanted)
    starts = [s for s in pairs if s not in set(pairs.values())]
    for start in starts:
        at = start
        while at in pairs:
            at = pairs[at]
        pairs[at] = start
    for i in range(count):
        pairs.setdefault(i, i)
    assert sorted(pairs.values()) == list(range(count))
    return sorted(pairs.items())


class Piece:
    def __init__(self, data, source):
        self.data, self.source = data, source

    def move(self, pairs):
        source = list(self.source)
        for s, t in pairs:
            source[t] = self.source[s]
        return Piece(lax.ppermute(self.data, "seq", pairs), source)


def rotated(x, cosine, sine):
    return x * cosine + pltpu.roll(x, HEAD_DIM // 2, 1) * sine


def prepare_kernel(k_ref, v_ref, cos_ref, sin_ref, kv_ref):
    width = KV_HEADS * HEAD_DIM
    cosine, sine = cos_ref[...], sin_ref[...]
    for g in range(KV_HEADS):
        cols = slice(g * HEAD_DIM, (g + 1) * HEAD_DIM)
        kv_ref[:, cols] = rotated(k_ref[:, cols].astype(jnp.float32), cosine, sine).astype(jnp.bfloat16)
    kv_ref[:, width:] = v_ref[...]


def prepare(keys, values, cosine, sine):
    rows = keys.shape[0]
    return pl.pallas_call(
        prepare_kernel,
        out_shape=jax.ShapeDtypeStruct((rows, 2 * KV_HEADS * HEAD_DIM), jnp.bfloat16),
        cost_estimate=pl.CostEstimate(flops=10**6, bytes_accessed=6 * 10**5, transcendentals=0),
        compiler_params=pltpu.CompilerParams(vmem_limit_bytes=VMEM_LIMIT),
        name="prepare",
    )(keys, values, cosine, sine)


def attend_kernel(count, first, last, *refs):
    refs = list(refs)
    take = lambda n: [refs.pop(0) for _ in range(n)]
    lengths_ref, bases_ref, q_ref = take(3)
    kv_refs = take(count)
    if first:
        cos_ref, sin_ref = take(2)
    else:
        max_in, sum_in, acc_in = take(3)
    if last:
        (out_ref,) = take(1)
    elif first:
        q_out, max_out, sum_out, acc_out = take(4)
    else:
        max_out, sum_out, acc_out = take(3)
    score_ref, weight_ref, bias_ref = take(3)
    if last:
        sum_out, acc_out = take(2)

    me = lax.axis_index("seq")
    rows = kv_refs[0].shape[0]
    width = KV_HEADS * HEAD_DIM
    tall = GROUP * rows

    own = me * rows + lax.broadcasted_iota(jnp.int32, (rows, rows), 1)
    start = jnp.zeros((rows, rows), jnp.int32)
    end = 0
    for d in range(lengths_ref.shape[0]):
        end = end + lengths_ref[d]
        start = start + jnp.where(own >= end, lengths_ref[d], 0)
    for b in range(count):
        place = bases_ref[b, me] + lax.broadcasted_iota(jnp.int32, (rows, rows), 0)
        allowed = (place >= start) & (place <= own)
        bias_ref[b * rows:(b + 1) * rows, :] = jnp.where(allowed, 0.0, MASKED).astype(jnp.bfloat16)
    same = lax.broadcasted_iota(jnp.int32, (rows, rows), 0) == lax.broadcasted_iota(jnp.int32, (rows, rows), 1)
    unit = jnp.where(same, 1.0, 0.0).astype(jnp.bfloat16)
    units = jnp.concatenate([unit] * GROUP, axis=0)

    if first:
        cosine, sine = cos_ref[...], sin_ref[...]
        for h in range(HEADS):
            head = q_ref[:, h * HEAD_DIM:(h + 1) * HEAD_DIM].astype(jnp.float32)
            g, at = h // GROUP, h % GROUP * rows
            q_out[g, at:at + rows] = rotated(head, cosine, sine).astype(jnp.bfloat16)
        q_ref = q_out

    def score(g):
        q = jnp.concatenate([q_ref[g], units], axis=1)
        k = jnp.concatenate([r[:, g * HEAD_DIM:(g + 1) * HEAD_DIM] for r in kv_refs], axis=0)
        k = jnp.concatenate([k, bias_ref[...]], axis=1)
        return lax.dot_general(q, k, (((1,), (1,)), ((), ())), preferred_element_type=jnp.float32)

    score_ref[0] = score(0)
    for g in range(KV_HEADS):
        slot = g % 2
        if g + 1 < KV_HEADS:
            score_ref[1 - slot] = score(g + 1)
        v = jnp.concatenate(
            [r[:, width + g * HEAD_DIM:width + (g + 1) * HEAD_DIM] for r in kv_refs], axis=0
        )
        for at in range(0, tall, SLAB):
            here = slice(at, at + SLAB)
            raw = score_ref[slot, here]
            top = jnp.max(raw, axis=1, keepdims=True) * SCORE_SCALE
            if first:
                top = jnp.broadcast_to(top, (SLAB, HEAD_DIM))
                total = None
            else:
                old = max_in[g, here]
                top = jnp.maximum(old, top)
                shrink = jnp.exp2(old - top)
                total = sum_in[g, here] * shrink
                acc_out[g, here] = acc_in[g, here] * shrink
            for b in range(count):
                cols = slice(b * rows, (b + 1) * rows)
                weight = jnp.exp2(raw[:, cols] * SCORE_SCALE - top)
                total = weight if total is None else total + weight
                weight_ref[slot, here, cols] = weight.astype(jnp.bfloat16)
            sum_out[g, here] = total
            if not last:
                max_out[g, here] = top
        mixed = jnp.dot(weight_ref[slot], v, preferred_element_type=jnp.float32)
        if first:
            acc_out[g] = mixed
        elif not last:
            acc_out[g] += mixed
        else:
            for h in range(GROUP):
                here = slice(h * rows, (h + 1) * rows)
                cols = slice((g * GROUP + h) * HEAD_DIM, (g * GROUP + h + 1) * HEAD_DIM)
                total = jnp.sum(sum_out[g, here], axis=1, keepdims=True)
                out_ref[:, cols] = ((acc_out[g, here] + mixed[here]) / total).astype(jnp.bfloat16)


def attend(lengths, q, pieces, table, state=None, turn=None, last=False):
    first = state is None
    count = len(pieces)
    rows = pieces[0].data.shape[0]
    assert rows == HEAD_DIM
    stacked = (KV_HEADS, GROUP * rows, HEAD_DIM)
    smem = pl.BlockSpec(memory_space=pltpu.SMEM)
    vmem = pl.BlockSpec(memory_space=pltpu.VMEM)
    args = [lengths, table, q] + [p.data for p in pieces]
    aliases = {}
    if first:
        args += list(turn)
    else:
        if not last:
            aliases = {len(args) + n: n for n in range(3)}
        args += list(state)
    held = jax.ShapeDtypeStruct(stacked, jnp.float32)
    if last:
        out_shape = [jax.ShapeDtypeStruct((rows, HEADS * HEAD_DIM), jnp.bfloat16)]
    elif first:
        out_shape = [jax.ShapeDtypeStruct(stacked, jnp.bfloat16)] + [held] * 3
    else:
        out_shape = [held] * 3
    scratch = [
        pltpu.VMEM((2, GROUP * rows, count * rows), jnp.float32),
        pltpu.VMEM((2, GROUP * rows, count * rows), jnp.bfloat16),
        pltpu.VMEM((count * rows, rows), jnp.bfloat16),
    ]
    if last:
        scratch += [pltpu.VMEM(stacked, jnp.float32)] * 2
    out = pl.pallas_call(
        functools.partial(attend_kernel, count, first, last),
        out_shape=out_shape,
        in_specs=[smem, smem] + [vmem] * (len(args) - 2),
        out_specs=[vmem] * len(out_shape),
        scratch_shapes=scratch,
        input_output_aliases=aliases,
        cost_estimate=pl.CostEstimate(
            flops=4 * rows * HEADS * count * rows * HEAD_DIM,
            bytes_accessed=4 * 10**6,
            transcendentals=rows * HEADS * count * rows,
        ),
        compiler_params=pltpu.CompilerParams(vmem_limit_bytes=VMEM_LIMIT),
    )(*args)
    return out[0] if last else out


def turns(rows, doc_lengths):
    half = HEAD_DIM // 2
    place = lax.axis_index("seq") * rows + jnp.arange(rows, dtype=jnp.int32)
    start = jnp.zeros_like(place)
    end = jnp.int32(0)
    for d in range(doc_lengths.shape[0]):
        end = end + doc_lengths[d]
        start = start + jnp.where(place >= end, doc_lengths[d], 0)
    freq = jnp.power(jnp.float32(ROPE_BASE), -2.0 * jnp.arange(half, dtype=jnp.float32) / HEAD_DIM)
    angle = (place - start).astype(jnp.float32)[:, None] * freq[None, :]
    cosine, sine = jnp.cos(angle), jnp.sin(angle)
    return jnp.concatenate([cosine, cosine], axis=1), jnp.concatenate([-sine, sine], axis=1)


def per_device(count, queries, keys, values, doc_lengths):
    rows = queries.shape[0]
    most_doc = rows * count * 5 // 8
    reach = -(-(most_doc - 1) // rows)
    chip_reach = -(-(most_doc - 1) // (2 * rows))

    def closed(shift, keep):
        return cycles({i: i + shift for i in range(count) if i + shift < count and keep(i)}, count)

    sibling = [(i, i ^ 1) for i in range(count)]
    across = [(i, i ^ 2) for i in range(count)]
    turn = turns(rows, doc_lengths)
    own = Piece(prepare(keys, values, *turn), list(range(count)))
    late = own.move(sibling)
    stages = [[own]]
    a, before = own, None
    half_reach = chip_reach // 2
    for s in range(1, half_reach + 1):
        b = a.move(across)
        a = a.move(closed(4, lambda i: i >= 4 * (s - 1)))
        stage = [a, b, a.move(sibling), b.move(sibling)]
        stages.append(([late] if s == 1 else []) + stage)
        before = b
    if chip_reach % 2:
        near = 4 * half_reach
        c = before.move(closed(4, lambda i: not i & 2 and i >= near - 4))
        a = a.move(closed(2, lambda i: i >= near))
        stages += [[a, c], [a.move(sibling), c.move(sibling)]]
    else:
        b = a.move(across)
        stages += [[b], [b.move(sibling)]]

    seen = [set() for _ in range(count)]
    tables = []
    for pieces in stages:
        table = np.full((len(pieces), count), NOWHERE, np.int32)
        for b, piece in enumerate(pieces):
            for i in range(count):
                j = piece.source[i]
                if i - reach <= j <= i and j not in seen[i]:
                    seen[i].add(j)
                    table[b, i] = j * rows
        tables.append(jnp.asarray(table))
    for i in range(count):
        assert seen[i] == set(range(max(0, i - reach), i + 1))

    state = None
    for n, pieces in enumerate(stages):
        if n == 0:
            q, *state = attend(doc_lengths, queries, pieces, tables[n], turn=turn)
        elif n < len(stages) - 1:
            state = attend(doc_lengths, q, pieces, tables[n], state=state)
        else:
            return attend(doc_lengths, q, pieces, tables[n], state=state, last=True)


def solution(mesh):
    count = mesh.shape["seq"]

    def body(*args):
        return per_device(count, *args)

    return jax.shard_map(
        body,
        mesh=mesh,
        in_specs=(
            P(("grp", "seq"), None),
            P(("grp", "seq"), None),
            P(("grp", "seq"), None),
            P("grp"),
        ),
        out_specs=P(("grp", "seq"), None),
        check_vma=False,
    )
```

```python
import functools

import jax
import jax.numpy as jnp
from jax import lax
from jax.experimental import pallas as pl
from jax.experimental.pallas import tpu as pltpu
from jax.sharding import PartitionSpec as P


HEADS = 28
KV_HEADS = 4
HEAD_DIM = 128
GROUP = HEADS // KV_HEADS
ROPE_BASE = 1000000.0
SCORE_SCALE = HEAD_DIM ** (-0.5) * 1.4426950408889634
MASKED = -65536.0
NOWHERE = 1 << 28
VMEM_LIMIT = 24 * 1024 * 1024
SLAB = 32


def cycles(wanted, count):
    pairs = dict(wanted)
    starts = [s for s in pairs if s not in set(pairs.values())]
    for start in starts:
        at = start
        while at in pairs:
            at = pairs[at]
        pairs[at] = start
    for i in range(count):
        pairs.setdefault(i, i)
    assert sorted(pairs.values()) == list(range(count))
    return sorted(pairs.items())


class Piece:
    def __init__(self, data, source):
        self.data, self.source = data, source

    def move(self, pairs):
        source = list(self.source)
        for s, t in pairs:
            source[t] = self.source[s]
        return Piece(lax.ppermute(self.data, "seq", pairs), source)


def rotated(x, cosine, sine):
    return x * cosine + pltpu.roll(x, HEAD_DIM // 2, 1) * sine


def in_hbm(x):
    return pltpu.with_memory_space_constraint(x, pltpu.HBM)


def lanes_iota(shape, dim):
    return lax.broadcasted_iota(jnp.int32, shape, dim)


def doc_starts(place, lengths_ref):
    start = jnp.zeros_like(place)
    end = 0
    for d in range(lengths_ref.shape[0]):
        end = end + lengths_ref[d]
        start = start + jnp.where(place >= end, lengths_ref[d], 0)
    return start


def prepare_kernel(freq_ref, lengths_hbm, k_hbm, v_hbm, kv_ref, cos_ref, sin_ref, lengths_ref, k_ref, sems):
    rows = k_ref.shape[0]
    width = KV_HEADS * HEAD_DIM
    copies = [
        pltpu.make_async_copy(lengths_hbm, lengths_ref, sems.at[0]),
        pltpu.make_async_copy(k_hbm, k_ref, sems.at[1]),
        pltpu.make_async_copy(v_hbm, kv_ref.at[:, pl.ds(width, width)], sems.at[2]),
    ]
    for copy in copies:
        copy.start()
    copies[0].wait()
    shape = (rows, HEAD_DIM)
    place = lax.axis_index("seq") * rows + lanes_iota(shape, 0)
    within = (place - doc_starts(place, lengths_ref)).astype(jnp.float32)
    angle = within * freq_ref[...]
    cosine = jnp.cos(angle)
    sine = jnp.sin(angle)
    sine = jnp.where(lanes_iota(shape, 1) < HEAD_DIM // 2, -sine, sine)
    cos_ref[...] = cosine
    sin_ref[...] = sine
    copies[1].wait()
    for g in range(KV_HEADS):
        cols = slice(g * HEAD_DIM, (g + 1) * HEAD_DIM)
        kv_ref[:, cols] = rotated(k_ref[:, cols].astype(jnp.float32), cosine, sine).astype(jnp.bfloat16)
    copies[2].wait()


def prepare(lengths, keys, values):
    rows = keys.shape[0]
    half = HEAD_DIM // 2
    lane = jnp.arange(HEAD_DIM, dtype=jnp.int32)[None, :]
    step = jnp.where(lane < half, lane, lane - half).astype(jnp.float32)
    freq = jnp.power(jnp.float32(ROPE_BASE), -2.0 * step / HEAD_DIM)
    vmem = pl.BlockSpec(memory_space=pltpu.VMEM)
    hbm = pl.BlockSpec(memory_space=pltpu.HBM)
    turn = jax.ShapeDtypeStruct((rows, HEAD_DIM), jnp.float32)
    return pl.pallas_call(
        prepare_kernel,
        out_shape=[jax.ShapeDtypeStruct((rows, 2 * KV_HEADS * HEAD_DIM), jnp.bfloat16), turn, turn],
        in_specs=[vmem, hbm, hbm, hbm],
        out_specs=[vmem] * 3,
        scratch_shapes=[
            pltpu.SMEM(lengths.shape, jnp.int32),
            pltpu.VMEM(keys.shape, keys.dtype),
            pltpu.SemaphoreType.DMA((3,)),
        ],
        cost_estimate=pl.CostEstimate(flops=10**6, bytes_accessed=6 * 10**5, transcendentals=0),
        compiler_params=pltpu.CompilerParams(vmem_limit_bytes=VMEM_LIMIT),
        name="prepare",
    )(freq, in_hbm(lengths), in_hbm(keys), in_hbm(values))


def attend_kernel(count, first, last, places, *refs):
    refs = list(refs)
    take = lambda n: [refs.pop(0) for _ in range(n)]
    if first:
        lengths_hbm, q_hbm, cos_ref, sin_ref = take(4)
        kv_refs = take(count)
        q_ref, max_out, sum_out, acc_out = take(4)
        all_bias = take(len(places))
        bias_ref = all_bias[0]
    else:
        q_ref, bias_ref = take(2)
        kv_refs = take(count)
        max_in, sum_in, acc_in = take(3)
        if last:
            (out_ref,) = take(1)
        else:
            max_out, sum_out, acc_out = take(3)
    score_ref, weight_ref = take(2)
    if last:
        sum_out, acc_out = take(2)
    if first:
        lengths_ref, q_raw, sems = take(3)

    rows = kv_refs[0].shape[0]
    width = KV_HEADS * HEAD_DIM
    tall = GROUP * rows
    square = (rows, rows)

    if first:
        copies = [
            pltpu.make_async_copy(lengths_hbm, lengths_ref, sems.at[0]),
            pltpu.make_async_copy(q_hbm, q_raw, sems.at[1]),
        ]
        for copy in copies:
            copy.start()
        copies[0].wait()
        me = lax.axis_index("seq")
        own = me * rows + lanes_iota((8, rows), 1)
        start = jnp.broadcast_to(doc_starts(own, lengths_ref)[:1], square)
        own = me * rows + lanes_iota(square, 1)
        for n, stage in enumerate(places):
            for b, bases in enumerate(stage):
                base = jnp.int32(NOWHERE)
                for i, value in enumerate(bases):
                    if value != NOWHERE:
                        base = jnp.where(me == i, value, base)
                place = base + lanes_iota(square, 0)
                allowed = (place >= start) & (place <= own)
                bias = jnp.where(allowed, 0.0, MASKED).astype(jnp.bfloat16)
                all_bias[n][b * rows:(b + 1) * rows, :] = bias
        copies[1].wait()
        cosine, sine = cos_ref[...], sin_ref[...]
        for h in range(HEADS):
            head = q_raw[:, h * HEAD_DIM:(h + 1) * HEAD_DIM].astype(jnp.float32)
            g, at = h // GROUP, h % GROUP * rows
            q_ref[g, at:at + rows] = rotated(head, cosine, sine).astype(jnp.bfloat16)

    unit = jnp.where(lanes_iota(square, 0) == lanes_iota(square, 1), 1.0, 0.0).astype(jnp.bfloat16)
    units = jnp.concatenate([unit] * GROUP, axis=0)

    def score(g):
        q = jnp.concatenate([q_ref[g], units], axis=1)
        k = jnp.concatenate([r[:, g * HEAD_DIM:(g + 1) * HEAD_DIM] for r in kv_refs], axis=0)
        k = jnp.concatenate([k, bias_ref[...]], axis=1)
        return lax.dot_general(q, k, (((1,), (1,)), ((), ())), preferred_element_type=jnp.float32)

    score_ref[0] = score(0)
    for g in range(KV_HEADS):
        slot = g % 2
        if g + 1 < KV_HEADS:
            score_ref[1 - slot] = score(g + 1)
        v = jnp.concatenate(
            [r[:, width + g * HEAD_DIM:width + (g + 1) * HEAD_DIM] for r in kv_refs], axis=0
        )
        for at in range(0, tall, SLAB):
            here = slice(at, at + SLAB)
            raw = score_ref[slot, here]
            top = jnp.max(raw, axis=1, keepdims=True) * SCORE_SCALE
            if first:
                top = jnp.broadcast_to(top, (SLAB, HEAD_DIM))
                total = None
            else:
                old = max_in[g, here]
                top = jnp.maximum(old, top)
                shrink = jnp.exp2(old - top)
                total = sum_in[g, here] * shrink
                acc_out[g, here] = acc_in[g, here] * shrink
            for b in range(count):
                cols = slice(b * rows, (b + 1) * rows)
                weight = jnp.exp2(raw[:, cols] * SCORE_SCALE - top)
                total = weight if total is None else total + weight
                weight_ref[slot, here, cols] = weight.astype(jnp.bfloat16)
            sum_out[g, here] = total
            if not last:
                max_out[g, here] = top
        mixed = jnp.dot(weight_ref[slot], v, preferred_element_type=jnp.float32)
        if first:
            acc_out[g] = mixed
        elif not last:
            acc_out[g] += mixed
        else:
            for h in range(GROUP):
                here = slice(h * rows, (h + 1) * rows)
                cols = slice((g * GROUP + h) * HEAD_DIM, (g * GROUP + h + 1) * HEAD_DIM)
                total = jnp.sum(sum_out[g, here], axis=1, keepdims=True)
                out_ref[:, cols] = ((acc_out[g, here] + mixed[here]) / total).astype(jnp.bfloat16)


def attend(pieces, bias=None, q=None, state=None, start=None, last=False):
    first = start is not None
    count = len(pieces)
    rows = pieces[0].data.shape[0]
    assert rows == HEAD_DIM
    stacked = (KV_HEADS, GROUP * rows, HEAD_DIM)
    vmem = pl.BlockSpec(memory_space=pltpu.VMEM)
    hbm = pl.BlockSpec(memory_space=pltpu.HBM)
    data = [p.data for p in pieces]
    held = [jax.ShapeDtypeStruct(stacked, jnp.float32)] * 3
    scratch = [
        pltpu.VMEM((2, GROUP * rows, count * rows), jnp.float32),
        pltpu.VMEM((2, GROUP * rows, count * rows), jnp.bfloat16),
    ]
    aliases = {}
    places = None
    if first:
        lengths, queries, cosine, sine, places = start
        args = [in_hbm(lengths), in_hbm(queries), cosine, sine] + data
        in_specs = [hbm, hbm] + [vmem] * (2 + count)
        out_shape = [jax.ShapeDtypeStruct(stacked, jnp.bfloat16)] + held
        out_shape += [jax.ShapeDtypeStruct((len(stage) * rows, rows), jnp.bfloat16) for stage in places]
        scratch += [
            pltpu.SMEM(lengths.shape, jnp.int32),
            pltpu.VMEM(queries.shape, queries.dtype),
            pltpu.SemaphoreType.DMA((2,)),
        ]
    else:
        args = [q, bias] + data + list(state)
        in_specs = [vmem] * len(args)
        if last:
            out_shape = [jax.ShapeDtypeStruct((rows, HEADS * HEAD_DIM), jnp.bfloat16)]
            scratch += [pltpu.VMEM(stacked, jnp.float32)] * 2
        else:
            out_shape = held
            aliases = {2 + count + n: n for n in range(3)}
    return pl.pallas_call(
        functools.partial(attend_kernel, count, first, last, places),
        out_shape=out_shape,
        in_specs=in_specs,
        out_specs=[vmem] * len(out_shape),
        scratch_shapes=scratch,
        input_output_aliases=aliases,
        cost_estimate=pl.CostEstimate(
            flops=4 * rows * HEADS * count * rows * HEAD_DIM,
            bytes_accessed=4 * 10**6,
            transcendentals=rows * HEADS * count * rows,
        ),
        compiler_params=pltpu.CompilerParams(vmem_limit_bytes=VMEM_LIMIT),
    )(*args)


def block_reach(count):
    return -(-5 * count // 8)


def chip_reach_of(count):
    return -(-block_reach(count) // 2)


def per_device(count, queries, keys, values, doc_lengths):
    rows = queries.shape[0]
    reach, chip_reach = block_reach(count), chip_reach_of(count)

    def closed(shift, keep):
        return cycles({i: i + shift for i in range(count) if i + shift < count and keep(i)}, count)

    sibling = [(i, i ^ 1) for i in range(count)]
    across = [(i, i ^ 2) for i in range(count)]
    own, cosine, sine = prepare(doc_lengths, keys, values)
    own = Piece(own, list(range(count)))
    stages = [[own, own.move(sibling)]]
    a, before = own, None
    half_reach = chip_reach // 2
    for s in range(1, half_reach + 1):
        b = a.move(across)
        a = a.move(closed(4, lambda i: i >= 4 * (s - 1)))
        stages.append([a, b, a.move(sibling), b.move(sibling)])
        before = b
    if chip_reach % 2:
        near = 4 * half_reach
        c = before.move(closed(4, lambda i: not i & 2 and i >= near - 4))
        a = a.move(closed(2, lambda i: i >= near))
        stages += [[a, c], [a.move(sibling), c.move(sibling)]]
    else:
        b = a.move(across)
        stages += [[b], [b.move(sibling)]]

    seen = [set() for _ in range(count)]
    places = []
    for pieces in stages:
        table = [[NOWHERE] * count for _ in pieces]
        for b, piece in enumerate(pieces):
            for i in range(count):
                j = piece.source[i]
                if i - reach <= j <= i and j not in seen[i]:
                    seen[i].add(j)
                    table[b][i] = j * rows
        places.append(table)
    for i in range(count):
        assert seen[i] == set(range(max(0, i - reach), i + 1))

    for n, pieces in enumerate(stages):
        if n == 0:
            out = attend(pieces, start=(doc_lengths, queries, cosine, sine, places))
            q, state, bias = out[0], out[1:4], out[4:]
        else:
            state = attend(pieces, bias[n], q, state, last=n == len(stages) - 1)
    return state[0]


def solution(mesh):
    count = mesh.shape["seq"]

    def body(*args):
        return per_device(count, *args)

    return jax.shard_map(
        body,
        mesh=mesh,
        in_specs=(
            P(("grp", "seq"), None),
            P(("grp", "seq"), None),
            P(("grp", "seq"), None),
            P("grp"),
        ),
        out_specs=P(("grp", "seq"), None),
        check_vma=False,
    )
```

```python
import functools

import jax
import jax.numpy as jnp
from jax import lax
from jax.experimental import pallas as pl
from jax.experimental.pallas import tpu as pltpu
from jax.sharding import PartitionSpec as P


HEADS = 28
KV_HEADS = 4
HEAD_DIM = 128
GROUP = HEADS // KV_HEADS
ROPE_BASE = 1000000.0
SCORE_SCALE = HEAD_DIM ** (-0.5) * 1.4426950408889634
MASKED = -16384.0
NOWHERE = 1 << 28
VMEM_LIMIT = 24 * 1024 * 1024
SLAB = 32


def cycles(wanted, count):
    pairs = dict(wanted)
    starts = [s for s in pairs if s not in set(pairs.values())]
    for start in starts:
        at = start
        while at in pairs:
            at = pairs[at]
        pairs[at] = start
    for i in range(count):
        pairs.setdefault(i, i)
    assert sorted(pairs.values()) == list(range(count))
    return sorted(pairs.items())


class Piece:
    def __init__(self, data, source):
        self.data, self.source = data, source

    def move(self, pairs):
        source = list(self.source)
        for s, t in pairs:
            source[t] = self.source[s]
        return Piece(lax.ppermute(self.data, "seq", pairs), source)


def rotated(x, cosine, sine):
    return x * cosine + pltpu.roll(x, HEAD_DIM // 2, 1) * sine


def in_hbm(x):
    return pltpu.with_memory_space_constraint(x, pltpu.HBM)


def lanes_iota(shape, dim):
    return lax.broadcasted_iota(jnp.int32, shape, dim)


def doc_starts(place, lengths_ref):
    start = jnp.zeros_like(place)
    end = 0
    for d in range(lengths_ref.shape[0]):
        end = end + lengths_ref[d]
        start = start + jnp.where(place >= end, lengths_ref[d], 0)
    return start


def prepare_kernel(freq_ref, lengths_hbm, k_hbm, v_hbm, kv_ref, cos_ref, sin_ref, lengths_ref, k_ref, sems):
    rows = k_ref.shape[0]
    width = KV_HEADS * HEAD_DIM
    copies = [
        pltpu.make_async_copy(lengths_hbm, lengths_ref, sems.at[0]),
        pltpu.make_async_copy(k_hbm, k_ref, sems.at[1]),
        pltpu.make_async_copy(v_hbm, kv_ref.at[:, pl.ds(width, width)], sems.at[2]),
    ]
    for copy in copies:
        copy.start()
    copies[0].wait()
    shape = (rows, HEAD_DIM)
    place = lax.axis_index("seq") * rows + lanes_iota(shape, 0)
    within = (place - doc_starts(place, lengths_ref)).astype(jnp.float32)
    angle = within * freq_ref[...]
    cosine = jnp.cos(angle)
    sine = jnp.sin(angle)
    sine = jnp.where(lanes_iota(shape, 1) < HEAD_DIM // 2, -sine, sine)
    cos_ref[...] = cosine
    sin_ref[...] = sine
    copies[1].wait()
    for g in range(KV_HEADS):
        cols = slice(g * HEAD_DIM, (g + 1) * HEAD_DIM)
        kv_ref[:, cols] = rotated(k_ref[:, cols].astype(jnp.float32), cosine, sine).astype(jnp.bfloat16)
    copies[2].wait()


def prepare(lengths, keys, values):
    rows = keys.shape[0]
    half = HEAD_DIM // 2
    lane = jnp.arange(HEAD_DIM, dtype=jnp.int32)[None, :]
    step = jnp.where(lane < half, lane, lane - half).astype(jnp.float32)
    freq = jnp.power(jnp.float32(ROPE_BASE), -2.0 * step / HEAD_DIM)
    vmem = pl.BlockSpec(memory_space=pltpu.VMEM)
    hbm = pl.BlockSpec(memory_space=pltpu.HBM)
    turn = jax.ShapeDtypeStruct((rows, HEAD_DIM), jnp.float32)
    return pl.pallas_call(
        prepare_kernel,
        out_shape=[jax.ShapeDtypeStruct((rows, 2 * KV_HEADS * HEAD_DIM), jnp.bfloat16), turn, turn],
        in_specs=[vmem, hbm, hbm, hbm],
        out_specs=[vmem] * 3,
        scratch_shapes=[
            pltpu.SMEM(lengths.shape, jnp.int32),
            pltpu.VMEM(keys.shape, keys.dtype),
            pltpu.SemaphoreType.DMA((3,)),
        ],
        cost_estimate=pl.CostEstimate(flops=10**6, bytes_accessed=6 * 10**5, transcendentals=0),
        compiler_params=pltpu.CompilerParams(vmem_limit_bytes=VMEM_LIMIT),
        name="prepare",
    )(freq, in_hbm(lengths), in_hbm(keys), in_hbm(values))


def turn_kernel(places, docs, lengths_hbm, q_hbm, cos_ref, sin_ref, *refs):
    q_ref, *rest = refs
    mask_refs, (lengths_ref, q_raw, sems) = rest[:-3], rest[-3:]
    rows = q_raw.shape[0]
    copies = [
        pltpu.make_async_copy(lengths_hbm, lengths_ref, sems.at[0]),
        pltpu.make_async_copy(q_hbm, q_raw, sems.at[1]),
    ]
    for copy in copies:
        copy.start()
    copies[0].wait()
    me = lax.axis_index("seq")
    square = (rows, HEAD_DIM)
    row, lane = lanes_iota(square, 0), lanes_iota(square, 1)
    first = jnp.full((8, HEAD_DIM), NOWHERE, jnp.int32)
    after = first
    end = 0
    for d in range(docs):
        here = lanes_iota((8, HEAD_DIM), 1) == d
        first = jnp.where(here, end, first)
        end = end + lengths_ref[d]
        after = jnp.where(here, end, after)
    first = jnp.broadcast_to(first[:1], square)
    after = jnp.broadcast_to(after[:1], square)
    for n, stage in enumerate(places):
        for b, bases in enumerate(stage):
            place = block_base(bases, me) + row
            member = (place >= first) & (place < after)
            mask_refs[n][b * rows:(b + 1) * rows, :] = jnp.where(member, 0.0, MASKED).astype(jnp.bfloat16)
    place = me * rows + row
    own_doc = jnp.where((place >= first) & (place < after), 1.0, 0.0)
    copies[1].wait()
    cosine, sine = cos_ref[...], sin_ref[...]
    for h in range(HEADS):
        head = q_raw[:, h * HEAD_DIM:(h + 1) * HEAD_DIM].astype(jnp.float32)
        g, at = h // GROUP, h % GROUP * rows
        turned = rotated(head, cosine, sine).astype(jnp.bfloat16).astype(jnp.float32) * SCORE_SCALE
        coarse = turned.astype(jnp.bfloat16)
        fine = turned - coarse.astype(jnp.float32)
        q_ref[g, at:at + rows, :HEAD_DIM] = coarse
        q_ref[g, at:at + rows, HEAD_DIM:] = jnp.where(lane < docs, own_doc, fine).astype(jnp.bfloat16)


def block_base(bases, me):
    base = jnp.int32(NOWHERE)
    for i, value in enumerate(bases):
        if value != NOWHERE:
            base = jnp.where(me == i, value, base)
    return base


def turn_queries(lengths, queries, cosine, sine, places):
    rows = queries.shape[0]
    assert rows == HEAD_DIM
    vmem = pl.BlockSpec(memory_space=pltpu.VMEM)
    hbm = pl.BlockSpec(memory_space=pltpu.HBM)
    out_shape = [jax.ShapeDtypeStruct((KV_HEADS, GROUP * rows, 2 * HEAD_DIM), jnp.bfloat16)]
    out_shape += [jax.ShapeDtypeStruct((len(stage) * rows, HEAD_DIM), jnp.bfloat16) for stage in places]
    return pl.pallas_call(
        functools.partial(turn_kernel, places, lengths.shape[0]),
        out_shape=out_shape,
        in_specs=[hbm, hbm, vmem, vmem],
        out_specs=[vmem] * len(out_shape),
        scratch_shapes=[
            pltpu.SMEM(lengths.shape, jnp.int32),
            pltpu.VMEM(queries.shape, queries.dtype),
            pltpu.SemaphoreType.DMA((2,)),
        ],
        cost_estimate=pl.CostEstimate(flops=10**8, bytes_accessed=4 * 10**6, transcendentals=0),
        compiler_params=pltpu.CompilerParams(vmem_limit_bytes=VMEM_LIMIT),
        name="turn_queries",
    )(in_hbm(lengths), in_hbm(queries), cosine, sine)


def attend_kernel(count, docs, first, last, users, *refs):
    refs = list(refs)
    take = lambda n: [refs.pop(0) for _ in range(n)]
    q_ref, mask_ref = take(2)
    kv_refs = take(count)
    if not first:
        max_in, sum_in, acc_in = take(3)
    if last:
        (out_ref,) = take(1)
    else:
        max_out, sum_out, acc_out = take(3)
    score_ref, shrink_ref = take(2)

    rows = kv_refs[0].shape[0]
    width = KV_HEADS * HEAD_DIM
    tall = GROUP * rows
    key_lane = lanes_iota((count * rows, HEAD_DIM), 1)
    ones = jnp.ones((count * rows, HEAD_DIM), jnp.bfloat16)

    def body():
        def score(g):
            k = jnp.concatenate([r[:, g * HEAD_DIM:(g + 1) * HEAD_DIM] for r in kv_refs], axis=0)
            k = jnp.concatenate([k, jnp.where(key_lane < docs, mask_ref[...], k)], axis=1)
            return lax.dot_general(q_ref[g], k, (((1,), (1,)), ((), ())), preferred_element_type=jnp.float32)

        score_ref[0] = score(0)
        for g in range(KV_HEADS):
            slot = g % 2
            if g + 1 < KV_HEADS:
                score_ref[1 - slot] = score(g + 1)
            v = jnp.concatenate(
                [r[:, width + g * HEAD_DIM:width + (g + 1) * HEAD_DIM] for r in kv_refs], axis=0
            )
            weights = []
            for at in range(0, tall, SLAB):
                here = slice(at, at + SLAB)
                scores = score_ref[slot, here]
                if first:
                    shape = (SLAB, count * rows)
                    after = lanes_iota(shape, 1) - lanes_iota(shape, 0) > at % rows
                    after &= lanes_iota(shape, 1) < rows
                    scores = jnp.where(after, MASKED, scores)
                    top = jnp.max(scores, axis=1, keepdims=True)
                    top = jnp.broadcast_to(top, (SLAB, HEAD_DIM))
                else:
                    old = max_in[g, here]
                    top = jnp.maximum(old, jnp.max(scores, axis=1, keepdims=True))
                    shrink_ref[slot, here] = jnp.exp2(old - top)
                if not last:
                    max_out[g, here] = top
                parts = [
                    jnp.exp2(scores[:, b * rows:(b + 1) * rows] - top).astype(jnp.bfloat16)
                    for b in range(count)
                ]
                weights.append(jnp.concatenate(parts, axis=1))
            mixed = jnp.dot(
                jnp.concatenate(weights, axis=0),
                jnp.concatenate([v, ones], axis=1),
                preferred_element_type=jnp.float32,
            )
            for at in range(0, tall, SLAB):
                here = slice(at, at + SLAB)
                acc, total = mixed[here, :HEAD_DIM], mixed[here, HEAD_DIM:]
                if not first:
                    shrink = shrink_ref[slot, here]
                    acc = acc_in[g, here] * shrink + acc
                    total = sum_in[g, here] * shrink + total
                if last:
                    head, row = g * GROUP + at // rows, at % rows
                    cols = slice(head * HEAD_DIM, (head + 1) * HEAD_DIM)
                    out_ref[row:row + SLAB, cols] = (acc / total).astype(jnp.bfloat16)
                else:
                    acc_out[g, here] = acc
                    sum_out[g, here] = total

    if first or last:
        body()
    else:
        me = lax.axis_index("seq")
        wanted = jnp.bool_(False)
        for i in users:
            wanted |= me == i
        pl.when(wanted)(body)


def attend(pieces, docs, places, q, mask, state=None, last=False):
    first = state is None
    count = len(pieces)
    rows = pieces[0].data.shape[0]
    stacked = (KV_HEADS, GROUP * rows, HEAD_DIM)
    vmem = pl.BlockSpec(memory_space=pltpu.VMEM)
    args = [q, mask] + [p.data for p in pieces] + ([] if first else list(state))
    if last:
        out_shape = [jax.ShapeDtypeStruct((rows, HEADS * HEAD_DIM), jnp.bfloat16)]
    else:
        out_shape = [jax.ShapeDtypeStruct(stacked, jnp.float32)] * 3
    users = [i for i in range(len(places[0])) if any(bases[i] != NOWHERE for bases in places)]
    return pl.pallas_call(
        functools.partial(attend_kernel, count, docs, first, last, users),
        out_shape=out_shape,
        in_specs=[vmem] * len(args),
        out_specs=[vmem] * len(out_shape),
        scratch_shapes=[
            pltpu.VMEM((2, GROUP * rows, count * rows), jnp.float32),
            pltpu.VMEM((2, GROUP * rows, HEAD_DIM), jnp.float32),
        ],
        input_output_aliases={} if first or last else {2 + count + n: n for n in range(3)},
        cost_estimate=pl.CostEstimate(
            flops=4 * rows * HEADS * count * rows * HEAD_DIM,
            bytes_accessed=4 * 10**6,
            transcendentals=rows * HEADS * count * rows,
        ),
        compiler_params=pltpu.CompilerParams(vmem_limit_bytes=VMEM_LIMIT),
    )(*args)


def block_reach(count):
    return -(-5 * count // 8)


def chip_reach_of(count):
    return -(-block_reach(count) // 2)


def per_device(count, queries, keys, values, doc_lengths):
    rows = queries.shape[0]
    reach, chip_reach = block_reach(count), chip_reach_of(count)

    def closed(shift, keep):
        return cycles({i: i + shift for i in range(count) if i + shift < count and keep(i)}, count)

    sibling = [(i, i ^ 1) for i in range(count)]
    across = [(i, i ^ 2) for i in range(count)]
    own, cosine, sine = prepare(doc_lengths, keys, values)
    own = Piece(own, list(range(count)))
    stages = [[own, own.move(sibling)]]
    a, before, late = own, None, []
    half_reach = chip_reach // 2
    for s in range(1, half_reach + 1):
        b = a.move(across)
        a = a.move(closed(4, lambda i: i >= 4 * (s - 1)))
        stages.append(late + [a, b])
        late = [a.move(sibling), b.move(sibling)]
        before = b
    if chip_reach % 2:
        near = 4 * half_reach
        c = before.move(closed(4, lambda i: not i & 2 and i >= near - 4))
        a = a.move(closed(2, lambda i: i >= near))
        stages += [late + [a, c], [a.move(sibling), c.move(sibling)]]
    else:
        b = a.move(across)
        stages += [late + [b], [b.move(sibling)]]

    seen = [set() for _ in range(count)]
    places = []
    for pieces in stages:
        table = [[NOWHERE] * count for _ in pieces]
        for b, piece in enumerate(pieces):
            for i in range(count):
                j = piece.source[i]
                if i - reach <= j <= i and j not in seen[i]:
                    seen[i].add(j)
                    table[b][i] = j * rows
        places.append(table)
    for i in range(count):
        assert seen[i] == set(range(max(0, i - reach), i + 1))

    q, *masks = turn_queries(doc_lengths, queries, cosine, sine, places)
    state, docs = None, doc_lengths.shape[0]
    for n, pieces in enumerate(stages):
        state = attend(pieces, docs, places[n], q, masks[n], state, last=n == len(stages) - 1)
    return state[0]


def solution(mesh):
    count = mesh.shape["seq"]

    def body(*args):
        return per_device(count, *args)

    return jax.shard_map(
        body,
        mesh=mesh,
        in_specs=(
            P(("grp", "seq"), None),
            P(("grp", "seq"), None),
            P(("grp", "seq"), None),
            P("grp"),
        ),
        out_specs=P(("grp", "seq"), None),
        check_vma=False,
    )
```

```python
import functools

import jax
import jax.numpy as jnp
from jax import lax
from jax.experimental import pallas as pl
from jax.experimental.pallas import tpu as pltpu
from jax.sharding import PartitionSpec as P


HEADS = 28
KV_HEADS = 4
HEAD_DIM = 128
GROUP = HEADS // KV_HEADS
ROPE_BASE = 1000000.0
SCORE_SCALE = HEAD_DIM ** (-0.5) * 1.4426950408889634
MASKED = -16384.0
NOWHERE = 1 << 28
VMEM_LIMIT = 24 * 1024 * 1024
SLAB = 32


class Held:
    def __init__(self, data, source):
        self.data, self.source = data, source

    def move(self, pairs):
        source = list(self.source)
        for s, t in pairs:
            source[t] = self.source[s]
        return Held(self.data if self.data is None else lax.ppermute(self.data, "seq", pairs), source)


def joined(a, b):
    return Held(join(a.data, b.data), [x + y for x, y in zip(a.source, b.source)])


def relay(own, chip_reach, kernel):
    count = len(own.source)

    def around(shift, first, side=None):
        span = count - first
        pairs = {}
        for i in range(count):
            if i < first or (side is not None and i & 2):
                pairs[i] = i ^ 1
            else:
                pairs[i] = first + (i - first + shift) % span
        if side is not None:
            for core in range(2):
                head, last = first + core, count - shift + core
                pairs[last], pairs[head + 2] = head + 2, head
        assert sorted(pairs.values()) == list(range(count))
        return sorted(pairs.items())

    sibling = [(i, i ^ 1) for i in range(count)]
    across = [(i, i ^ 2) for i in range(count)]

    def swapped(pieces):
        both = pieces[0] if len(pieces) == 1 else joined(*pieces)
        return both.move(sibling)

    full, odd = chip_reach // 2, chip_reach % 2
    a = own
    for s in range(1, full + 1):
        b = a.move(across)
        here = a.move(around(4, 4 * (s - 1)))
        if s == 1:
            kernel("k0", [own, own.move(sibling)])
        kernel("k%d" % s, [here, b])
        kernel("kd%d" % s, [swapped([here, b])])
        a = here
    stage = full + 1
    if odd:
        c = b.move(around(4, 4 * (full - 1), 0))
        pieces = [a.move(around(2, 4 * full)), c]
    else:
        pieces = [a.move(across)]
    kernel("k%d" % stage, pieces)
    kernel("last", [swapped(pieces)], True)


def rotated(x, cosine, sine):
    return x * cosine + pltpu.roll(x, HEAD_DIM // 2, 1) * sine


def in_hbm(x):
    return pltpu.with_memory_space_constraint(x, pltpu.HBM)


def lanes_iota(shape, dim):
    return lax.broadcasted_iota(jnp.int32, shape, dim)


def doc_starts(place, lengths_ref):
    start = jnp.zeros_like(place)
    end = 0
    for d in range(lengths_ref.shape[0]):
        end = end + lengths_ref[d]
        start = start + jnp.where(place >= end, lengths_ref[d], 0)
    return start


def prepare_kernel(freq_ref, lengths_hbm, k_hbm, v_hbm, kv_ref, cos_ref, sin_ref, lengths_ref, k_ref, sems):
    rows = k_ref.shape[0]
    width = KV_HEADS * HEAD_DIM
    copies = [
        pltpu.make_async_copy(lengths_hbm, lengths_ref, sems.at[0]),
        pltpu.make_async_copy(k_hbm, k_ref, sems.at[1]),
        pltpu.make_async_copy(v_hbm, kv_ref.at[:, pl.ds(width, width)], sems.at[2]),
    ]
    for copy in copies:
        copy.start()
    copies[0].wait()
    shape = (rows, HEAD_DIM)
    place = lax.axis_index("seq") * rows + lanes_iota(shape, 0)
    within = (place - doc_starts(place, lengths_ref)).astype(jnp.float32)
    angle = within * freq_ref[...]
    cosine = jnp.cos(angle)
    sine = jnp.sin(angle)
    sine = jnp.where(lanes_iota(shape, 1) < HEAD_DIM // 2, -sine, sine)
    cos_ref[...] = cosine
    sin_ref[...] = sine
    copies[1].wait()
    for g in range(KV_HEADS):
        cols = slice(g * HEAD_DIM, (g + 1) * HEAD_DIM)
        kv_ref[:, cols] = rotated(k_ref[:, cols].astype(jnp.float32), cosine, sine).astype(jnp.bfloat16)
    copies[2].wait()


def prepare(lengths, keys, values):
    rows = keys.shape[0]
    half = HEAD_DIM // 2
    lane = jnp.arange(HEAD_DIM, dtype=jnp.int32)[None, :]
    step = jnp.where(lane < half, lane, lane - half).astype(jnp.float32)
    freq = jnp.power(jnp.float32(ROPE_BASE), -2.0 * step / HEAD_DIM)
    vmem = pl.BlockSpec(memory_space=pltpu.VMEM)
    hbm = pl.BlockSpec(memory_space=pltpu.HBM)
    turn = jax.ShapeDtypeStruct((rows, HEAD_DIM), jnp.float32)
    return pl.pallas_call(
        prepare_kernel,
        out_shape=[jax.ShapeDtypeStruct((rows, 2 * KV_HEADS * HEAD_DIM), jnp.bfloat16), turn, turn],
        in_specs=[vmem, hbm, hbm, hbm],
        out_specs=[vmem] * 3,
        scratch_shapes=[
            pltpu.SMEM(lengths.shape, jnp.int32),
            pltpu.VMEM(keys.shape, keys.dtype),
            pltpu.SemaphoreType.DMA((3,)),
        ],
        cost_estimate=pl.CostEstimate(flops=10**6, bytes_accessed=6 * 10**5, transcendentals=0),
        compiler_params=pltpu.CompilerParams(vmem_limit_bytes=VMEM_LIMIT),
        name="prepare",
    )(freq, in_hbm(lengths), in_hbm(keys), in_hbm(values))


def turn_kernel(places, docs, lengths_hbm, q_hbm, cos_ref, sin_ref, *refs):
    q_ref, *rest = refs
    mask_refs, (lengths_ref, q_raw, sems) = rest[:-3], rest[-3:]
    rows = q_raw.shape[0]
    copies = [
        pltpu.make_async_copy(lengths_hbm, lengths_ref, sems.at[0]),
        pltpu.make_async_copy(q_hbm, q_raw, sems.at[1]),
    ]
    for copy in copies:
        copy.start()
    copies[0].wait()
    me = lax.axis_index("seq")
    square = (rows, HEAD_DIM)
    row, lane = lanes_iota(square, 0), lanes_iota(square, 1)
    first = jnp.full((8, HEAD_DIM), NOWHERE, jnp.int32)
    after = first
    end = 0
    for d in range(docs):
        here = lanes_iota((8, HEAD_DIM), 1) == d
        first = jnp.where(here, end, first)
        end = end + lengths_ref[d]
        after = jnp.where(here, end, after)
    first = jnp.broadcast_to(first[:1], square)
    after = jnp.broadcast_to(after[:1], square)
    for n, stage in enumerate(places):
        for b, bases in enumerate(stage):
            place = block_base(bases, me) + row
            member = (place >= first) & (place < after)
            mask_refs[n][b * rows:(b + 1) * rows, :] = jnp.where(member, 0.0, MASKED).astype(jnp.bfloat16)
    place = me * rows + row
    own_doc = jnp.where((place >= first) & (place < after), 1.0, 0.0)
    copies[1].wait()
    cosine, sine = cos_ref[...], sin_ref[...]
    for h in range(HEADS):
        head = q_raw[:, h * HEAD_DIM:(h + 1) * HEAD_DIM].astype(jnp.float32)
        g, at = h // GROUP, h % GROUP * rows
        turned = rotated(head, cosine, sine).astype(jnp.bfloat16).astype(jnp.float32) * SCORE_SCALE
        coarse = turned.astype(jnp.bfloat16)
        fine = turned - coarse.astype(jnp.float32)
        q_ref[g, at:at + rows, :HEAD_DIM] = coarse
        q_ref[g, at:at + rows, HEAD_DIM:] = jnp.where(lane < docs, own_doc, fine).astype(jnp.bfloat16)


def block_base(bases, me):
    base = jnp.int32(NOWHERE)
    for i, value in enumerate(bases):
        if value != NOWHERE:
            base = jnp.where(me == i, value, base)
    return base


def turn_queries(lengths, queries, cosine, sine, places):
    rows = queries.shape[0]
    assert rows == HEAD_DIM
    vmem = pl.BlockSpec(memory_space=pltpu.VMEM)
    hbm = pl.BlockSpec(memory_space=pltpu.HBM)
    out_shape = [jax.ShapeDtypeStruct((KV_HEADS, GROUP * rows, 2 * HEAD_DIM), jnp.bfloat16)]
    out_shape += [jax.ShapeDtypeStruct((len(stage) * rows, HEAD_DIM), jnp.bfloat16) for stage in places]
    return pl.pallas_call(
        functools.partial(turn_kernel, places, lengths.shape[0]),
        out_shape=out_shape,
        in_specs=[hbm, hbm, vmem, vmem],
        out_specs=[vmem] * len(out_shape),
        scratch_shapes=[
            pltpu.SMEM(lengths.shape, jnp.int32),
            pltpu.VMEM(queries.shape, queries.dtype),
            pltpu.SemaphoreType.DMA((2,)),
        ],
        cost_estimate=pl.CostEstimate(flops=10**8, bytes_accessed=4 * 10**6, transcendentals=0),
        compiler_params=pltpu.CompilerParams(vmem_limit_bytes=VMEM_LIMIT),
        name="turn_queries",
    )(in_hbm(lengths), in_hbm(queries), cosine, sine)


def attend_kernel(count, operands, docs, first, last, users, *refs):
    refs = list(refs)
    take = lambda n: [refs.pop(0) for _ in range(n)]
    q_ref, mask_ref = take(2)
    kv_refs = take(operands)
    if not first:
        max_in, sum_in, acc_in = take(3)
    if last:
        (out_ref,) = take(1)
    else:
        max_out, sum_out, acc_out = take(3)
    score_ref, shrink_ref = take(2)
    if last:
        out_hbm, (out_ref, sems) = out_ref, take(2)

    rows = score_ref.shape[2] // count
    kv_refs = [r.at[n:n + rows] for r in kv_refs for n in range(0, r.shape[0], rows)]
    width = KV_HEADS * HEAD_DIM
    tall = GROUP * rows
    key_lane = lanes_iota((count * rows, HEAD_DIM), 1)
    ones = jnp.ones((count * rows, HEAD_DIM), jnp.bfloat16)

    def body():
        def score(g):
            k = jnp.concatenate([r[:, g * HEAD_DIM:(g + 1) * HEAD_DIM] for r in kv_refs], axis=0)
            k = jnp.concatenate([k, jnp.where(key_lane < docs, mask_ref[...], k)], axis=1)
            return lax.dot_general(q_ref[g], k, (((1,), (1,)), ((), ())), preferred_element_type=jnp.float32)

        copies = []
        score_ref[0] = score(0)
        for g in range(KV_HEADS):
            slot = g % 2
            if g + 1 < KV_HEADS:
                score_ref[1 - slot] = score(g + 1)
            v = jnp.concatenate(
                [r[:, width + g * HEAD_DIM:width + (g + 1) * HEAD_DIM] for r in kv_refs], axis=0
            )
            weights = []
            for at in range(0, tall, SLAB):
                here = slice(at, at + SLAB)
                scores = score_ref[slot, here]
                if first:
                    shape = (SLAB, count * rows)
                    after = lanes_iota(shape, 1) - lanes_iota(shape, 0) > at % rows
                    after &= lanes_iota(shape, 1) < rows
                    scores = jnp.where(after, MASKED, scores)
                    top = jnp.max(scores, axis=1, keepdims=True)
                    top = jnp.broadcast_to(top, (SLAB, HEAD_DIM))
                else:
                    old = max_in[g, here]
                    top = jnp.maximum(old, jnp.max(scores, axis=1, keepdims=True))
                    shrink_ref[slot, here] = jnp.exp2(old - top)
                if not last:
                    max_out[g, here] = top
                parts = [
                    jnp.exp2(scores[:, b * rows:(b + 1) * rows] - top).astype(jnp.bfloat16)
                    for b in range(count)
                ]
                weights.append(jnp.concatenate(parts, axis=1))
            mixed = jnp.dot(
                jnp.concatenate(weights, axis=0),
                jnp.concatenate([v, ones], axis=1),
                preferred_element_type=jnp.float32,
            )
            for at in range(0, tall, SLAB):
                here = slice(at, at + SLAB)
                acc, total = mixed[here, :HEAD_DIM], mixed[here, HEAD_DIM:]
                if not first:
                    shrink = shrink_ref[slot, here]
                    acc = acc_in[g, here] * shrink + acc
                    total = sum_in[g, here] * shrink + total
                if last:
                    head, row = g * GROUP + at // rows, at % rows
                    cols = slice(head * HEAD_DIM, (head + 1) * HEAD_DIM)
                    out_ref[row:row + SLAB, cols] = (acc / total).astype(jnp.bfloat16)
                else:
                    acc_out[g, here] = acc
                    sum_out[g, here] = total
            if last:
                cols = pl.ds(g * GROUP * HEAD_DIM, GROUP * HEAD_DIM)
                copies.append(pltpu.make_async_copy(out_ref.at[:, cols], out_hbm.at[:, cols], sems.at[g]))
                copies[-1].start()
        for copy in copies:
            copy.wait()

    if first or last:
        body()
    else:
        me = lax.axis_index("seq")
        wanted = jnp.bool_(False)
        for i in users:
            wanted |= me == i
        pl.when(wanted)(body)


def attend(pieces, docs, places, q, mask, state=None, last=False):
    first = state is None
    count = len(places)
    rows = q.shape[1] // GROUP
    stacked = (KV_HEADS, GROUP * rows, HEAD_DIM)
    vmem = pl.BlockSpec(memory_space=pltpu.VMEM)
    args = [q, mask] + pieces + ([] if first else list(state))
    if last:
        out_shape = [jax.ShapeDtypeStruct((rows, HEADS * HEAD_DIM), jnp.bfloat16)]
    else:
        out_shape = [jax.ShapeDtypeStruct(stacked, jnp.float32)] * 3
    scratch = [
        pltpu.VMEM((2, GROUP * rows, count * rows), jnp.float32),
        pltpu.VMEM((2, GROUP * rows, HEAD_DIM), jnp.float32),
    ]
    if last:
        scratch += [pltpu.VMEM((rows, HEADS * HEAD_DIM), jnp.bfloat16), pltpu.SemaphoreType.DMA((KV_HEADS,))]
    users = [i for i in range(len(places[0])) if any(bases[i] != NOWHERE for bases in places)]
    return pl.pallas_call(
        functools.partial(attend_kernel, count, len(pieces), docs, first, last, users),
        out_shape=out_shape,
        in_specs=[vmem] * len(args),
        out_specs=[pl.BlockSpec(memory_space=pltpu.HBM)] if last else [vmem] * len(out_shape),
        scratch_shapes=scratch,
        input_output_aliases={} if first or last else {2 + len(pieces) + n: n for n in range(3)},
        cost_estimate=pl.CostEstimate(
            flops=4 * rows * HEADS * count * rows * HEAD_DIM,
            bytes_accessed=4 * 10**6,
            transcendentals=rows * HEADS * count * rows,
        ),
        compiler_params=pltpu.CompilerParams(vmem_limit_bytes=VMEM_LIMIT),
    )(*args)


def join_kernel(a_ref, b_ref, out_ref):
    rows = a_ref.shape[0]
    out_ref[:rows, :] = a_ref[...]
    out_ref[rows:, :] = b_ref[...]


def join(a, b):
    if a is None:
        return None
    vmem = pl.BlockSpec(memory_space=pltpu.VMEM)
    return pl.pallas_call(
        join_kernel,
        out_shape=jax.ShapeDtypeStruct((2 * a.shape[0], a.shape[1]), a.dtype),
        in_specs=[vmem] * 2,
        out_specs=vmem,
        cost_estimate=pl.CostEstimate(flops=10**5, bytes_accessed=10**6, transcendentals=0),
        compiler_params=pltpu.CompilerParams(vmem_limit_bytes=VMEM_LIMIT),
        name="join",
    )(a, b)


def block_reach(count):
    return -(-5 * count // 8)


def chip_reach_of(count):
    return -(-block_reach(count) // 2)


def per_device(count, queries, keys, values, doc_lengths):
    rows = queries.shape[0]
    reach, chip_reach = block_reach(count), chip_reach_of(count)

    seen = [set() for _ in range(count)]
    places = {}

    def place(name, pieces, last=False):
        table = []
        for piece in pieces:
            for b in range(len(piece.source[0])):
                bases = [NOWHERE] * count
                for i in range(count):
                    j = piece.source[i][b]
                    if i - reach <= j <= i and j not in seen[i]:
                        seen[i].add(j)
                        bases[i] = j * rows
                table.append(bases)
        places[name] = table

    source = [(i,) for i in range(count)]
    relay(Held(None, source), chip_reach, place)
    for i in range(count):
        assert seen[i] == set(range(max(0, i - reach), i + 1))

    own, cosine, sine = prepare(doc_lengths, keys, values)
    q, *masks = turn_queries(doc_lengths, queries, cosine, sine, list(places.values()))
    masks = dict(zip(places, masks))
    docs = doc_lengths.shape[0]
    held = {"state": None}

    def kernel(name, pieces, last=False):
        data = [p.data for p in pieces]
        held["state"] = attend(data, docs, places[name], q, masks[name], held["state"], last)

    relay(Held(own, source), chip_reach, kernel)
    return held["state"][0]


def solution(mesh):
    count = mesh.shape["seq"]

    def body(*args):
        return per_device(count, *args)

    return jax.shard_map(
        body,
        mesh=mesh,
        in_specs=(
            P(("grp", "seq"), None),
            P(("grp", "seq"), None),
            P(("grp", "seq"), None),
            P("grp"),
        ),
        out_specs=P(("grp", "seq"), None),
        check_vma=False,
    )
```

```python
import functools

import jax
import jax.numpy as jnp
from jax import lax
from jax.experimental import pallas as pl
from jax.experimental.pallas import tpu as pltpu
from jax.sharding import PartitionSpec as P


HEADS = 28
KV_HEADS = 4
HEAD_DIM = 128
GROUP = HEADS // KV_HEADS
ROPE_BASE = 1000000.0
SCORE_SCALE = HEAD_DIM ** (-0.5) * 1.4426950408889634
MASKED = -16384.0
NOWHERE = 1 << 28
VMEM_LIMIT = 24 * 1024 * 1024
SLAB = 32


class Held:
    def __init__(self, data, source):
        self.data, self.source = data, source

    def move(self, pairs):
        source = list(self.source)
        for s, t in pairs:
            source[t] = self.source[s]
        return Held(self.data if self.data is None else lax.ppermute(self.data, "seq", pairs), source)


def joined(a, b):
    return Held(join(a.data, b.data), [x + y for x, y in zip(a.source, b.source)])


def relay(own, chip_reach, kernel):
    count = len(own.source)

    def around(shift, first, narrow=False):
        span = count - first
        pairs = {}
        for i in range(count):
            if i < first or (narrow and i & 2):
                pairs[i] = i ^ 1
            else:
                pairs[i] = first + (i - first + shift) % span
        assert sorted(pairs.values()) == list(range(count))
        return sorted(pairs.items())

    sibling = [(i, i ^ 1) for i in range(count)]
    across = [(i, i ^ 2) for i in range(count)]

    def swapped(pieces):
        both = pieces[0] if len(pieces) == 1 else joined(*pieces)
        return both.move(sibling)

    full, odd = chip_reach // 2, chip_reach % 2
    a = own
    for s in range(1, full + 1):
        b = a.move(across)
        here = a.move(around(4, 4 * (s - 1)))
        if s == 1:
            kernel("k0", [own, own.move(sibling)])
        kernel("k%d" % s, [here, b])
        kernel("kd%d" % s, [swapped([here, b])])
        a = here
    stage = full + 1
    if odd:
        c = b.move(around(4, 4 * (full - 1), True))
        pieces = [a.move(around(2, 4 * full)), c]
    else:
        pieces = [a.move(across)]
    kernel("k%d" % stage, pieces)
    kernel("last", [swapped(pieces)], True)


def rotated(x, cosine, sine):
    return x * cosine + pltpu.roll(x, HEAD_DIM // 2, 1) * sine


def in_hbm(x):
    return pltpu.with_memory_space_constraint(x, pltpu.HBM)


def lanes_iota(shape, dim):
    return lax.broadcasted_iota(jnp.int32, shape, dim)


def doc_starts(place, lengths_ref):
    start = jnp.zeros_like(place)
    end = 0
    for d in range(lengths_ref.shape[0]):
        end = end + lengths_ref[d]
        start = start + jnp.where(place >= end, lengths_ref[d], 0)
    return start


def prepare_kernel(freq_ref, lengths_hbm, k_hbm, v_hbm, kv_ref, cos_ref, sin_ref, lengths_ref, k_ref, sems):
    rows = k_ref.shape[0]
    width = KV_HEADS * HEAD_DIM
    copies = [
        pltpu.make_async_copy(lengths_hbm, lengths_ref, sems.at[0]),
        pltpu.make_async_copy(k_hbm, k_ref, sems.at[1]),
        pltpu.make_async_copy(v_hbm, kv_ref.at[:, pl.ds(width, width)], sems.at[2]),
    ]
    for copy in copies:
        copy.start()
    copies[0].wait()
    shape = (rows, HEAD_DIM)
    place = lax.axis_index("seq") * rows + lanes_iota(shape, 0)
    within = (place - doc_starts(place, lengths_ref)).astype(jnp.float32)
    angle = within * freq_ref[...]
    cosine = jnp.cos(angle)
    sine = jnp.sin(angle)
    sine = jnp.where(lanes_iota(shape, 1) < HEAD_DIM // 2, -sine, sine)
    cos_ref[...] = cosine
    sin_ref[...] = sine
    copies[1].wait()
    for g in range(KV_HEADS):
        cols = slice(g * HEAD_DIM, (g + 1) * HEAD_DIM)
        kv_ref[:, cols] = rotated(k_ref[:, cols].astype(jnp.float32), cosine, sine).astype(jnp.bfloat16)
    copies[2].wait()


def prepare(lengths, keys, values):
    rows = keys.shape[0]
    half = HEAD_DIM // 2
    lane = jnp.arange(HEAD_DIM, dtype=jnp.int32)[None, :]
    step = jnp.where(lane < half, lane, lane - half).astype(jnp.float32)
    freq = jnp.power(jnp.float32(ROPE_BASE), -2.0 * step / HEAD_DIM)
    vmem = pl.BlockSpec(memory_space=pltpu.VMEM)
    hbm = pl.BlockSpec(memory_space=pltpu.HBM)
    turn = jax.ShapeDtypeStruct((rows, HEAD_DIM), jnp.float32)
    return pl.pallas_call(
        prepare_kernel,
        out_shape=[jax.ShapeDtypeStruct((rows, 2 * KV_HEADS * HEAD_DIM), jnp.bfloat16), turn, turn],
        in_specs=[vmem, hbm, hbm, hbm],
        out_specs=[vmem] * 3,
        scratch_shapes=[
            pltpu.SMEM(lengths.shape, jnp.int32),
            pltpu.VMEM(keys.shape, keys.dtype),
            pltpu.SemaphoreType.DMA((3,)),
        ],
        cost_estimate=pl.CostEstimate(flops=10**6, bytes_accessed=6 * 10**5, transcendentals=0),
        compiler_params=pltpu.CompilerParams(vmem_limit_bytes=VMEM_LIMIT),
        name="prepare",
    )(freq, in_hbm(lengths), in_hbm(keys), in_hbm(values))


def turn_kernel(places, docs, lengths_hbm, q_hbm, cos_ref, sin_ref, *refs):
    q_ref, *rest = refs
    mask_refs, (lengths_ref, q_raw, sems) = rest[:-3], rest[-3:]
    rows = q_raw.shape[0]
    copies = [
        pltpu.make_async_copy(lengths_hbm, lengths_ref, sems.at[0]),
        pltpu.make_async_copy(q_hbm, q_raw, sems.at[1]),
    ]
    for copy in copies:
        copy.start()
    copies[0].wait()
    me = lax.axis_index("seq")
    square = (rows, HEAD_DIM)
    row, lane = lanes_iota(square, 0), lanes_iota(square, 1)
    first = jnp.full((8, HEAD_DIM), NOWHERE, jnp.int32)
    after = first
    end = 0
    for d in range(docs):
        here = lanes_iota((8, HEAD_DIM), 1) == d
        first = jnp.where(here, end, first)
        end = end + lengths_ref[d]
        after = jnp.where(here, end, after)
    first = jnp.broadcast_to(first[:1], square)
    after = jnp.broadcast_to(after[:1], square)
    for n, stage in enumerate(places):
        for b, bases in enumerate(stage):
            place = block_base(bases, me) + row
            member = (place >= first) & (place < after)
            mask_refs[n][b * rows:(b + 1) * rows, :] = jnp.where(member, 0.0, MASKED).astype(jnp.bfloat16)
    place = me * rows + row
    own_doc = jnp.where((place >= first) & (place < after), 1.0, 0.0)
    copies[1].wait()
    cosine, sine = cos_ref[...], sin_ref[...]
    for h in range(HEADS):
        head = q_raw[:, h * HEAD_DIM:(h + 1) * HEAD_DIM].astype(jnp.float32)
        g, at = h // GROUP, h % GROUP * rows
        turned = rotated(head, cosine, sine).astype(jnp.bfloat16).astype(jnp.float32) * SCORE_SCALE
        coarse = turned.astype(jnp.bfloat16)
        fine = turned - coarse.astype(jnp.float32)
        q_ref[g, at:at + rows, :HEAD_DIM] = coarse
        q_ref[g, at:at + rows, HEAD_DIM:] = jnp.where(lane < docs, own_doc, fine).astype(jnp.bfloat16)


def block_base(bases, me):
    base = jnp.int32(NOWHERE)
    for i, value in enumerate(bases):
        if value != NOWHERE:
            base = jnp.where(me == i, value, base)
    return base


def turn_queries(lengths, queries, cosine, sine, places):
    rows = queries.shape[0]
    assert rows == HEAD_DIM
    vmem = pl.BlockSpec(memory_space=pltpu.VMEM)
    hbm = pl.BlockSpec(memory_space=pltpu.HBM)
    out_shape = [jax.ShapeDtypeStruct((KV_HEADS, GROUP * rows, 2 * HEAD_DIM), jnp.bfloat16)]
    out_shape += [jax.ShapeDtypeStruct((len(stage) * rows, HEAD_DIM), jnp.bfloat16) for stage in places]
    return pl.pallas_call(
        functools.partial(turn_kernel, places, lengths.shape[0]),
        out_shape=out_shape,
        in_specs=[hbm, hbm, vmem, vmem],
        out_specs=[vmem] * len(out_shape),
        scratch_shapes=[
            pltpu.SMEM(lengths.shape, jnp.int32),
            pltpu.VMEM(queries.shape, queries.dtype),
            pltpu.SemaphoreType.DMA((2,)),
        ],
        cost_estimate=pl.CostEstimate(flops=10**8, bytes_accessed=4 * 10**6, transcendentals=0),
        compiler_params=pltpu.CompilerParams(vmem_limit_bytes=VMEM_LIMIT),
        name="turn_queries",
    )(in_hbm(lengths), in_hbm(queries), cosine, sine)


def attend_kernel(count, operands, docs, first, last, users, *refs):
    refs = list(refs)
    take = lambda n: [refs.pop(0) for _ in range(n)]
    q_ref, mask_ref = take(2)
    kv_refs = take(operands)
    if not first:
        max_in, sum_in, acc_in = take(3)
    if last:
        (out_ref,) = take(1)
    else:
        max_out, sum_out, acc_out = take(3)
    score_ref, shrink_ref = take(2)
    if last:
        out_hbm, (out_ref, sems) = out_ref, take(2)

    rows = score_ref.shape[2] // count
    kv_refs = [r.at[n:n + rows] for r in kv_refs for n in range(0, r.shape[0], rows)]
    width = KV_HEADS * HEAD_DIM
    tall = GROUP * rows
    key_lane = lanes_iota((count * rows, HEAD_DIM), 1)
    ones = jnp.ones((count * rows, HEAD_DIM), jnp.bfloat16)

    def write(g, at, acc, total):
        head, row = g * GROUP + at // rows, at % rows
        cols = slice(head * HEAD_DIM, (head + 1) * HEAD_DIM)
        out_ref[row:row + SLAB, cols] = (acc / total).astype(jnp.bfloat16)

    def send(g):
        cols = pl.ds(g * GROUP * HEAD_DIM, GROUP * HEAD_DIM)
        copy = pltpu.make_async_copy(out_ref.at[:, cols], out_hbm.at[:, cols], sems.at[g])
        copy.start()
        return copy

    def finish(result):
        copies = []
        for g in range(KV_HEADS):
            for at in range(0, tall, SLAB):
                write(g, at, *result(g, slice(at, at + SLAB)))
            copies.append(send(g))
        for copy in copies:
            copy.wait()

    def body():
        def score(g):
            k = jnp.concatenate([r[:, g * HEAD_DIM:(g + 1) * HEAD_DIM] for r in kv_refs], axis=0)
            k = jnp.concatenate([k, jnp.where(key_lane < docs, mask_ref[...], k)], axis=1)
            return lax.dot_general(q_ref[g], k, (((1,), (1,)), ((), ())), preferred_element_type=jnp.float32)

        copies = []
        score_ref[0] = score(0)
        for g in range(KV_HEADS):
            slot = g % 2
            if g + 1 < KV_HEADS:
                score_ref[1 - slot] = score(g + 1)
            v = jnp.concatenate(
                [r[:, width + g * HEAD_DIM:width + (g + 1) * HEAD_DIM] for r in kv_refs], axis=0
            )
            weights = []
            for at in range(0, tall, SLAB):
                here = slice(at, at + SLAB)
                scores = score_ref[slot, here]
                if first:
                    shape = (SLAB, count * rows)
                    after = lanes_iota(shape, 1) - lanes_iota(shape, 0) > at % rows
                    after &= lanes_iota(shape, 1) < rows
                    scores = jnp.where(after, MASKED, scores)
                    top = jnp.max(scores, axis=1, keepdims=True)
                    top = jnp.broadcast_to(top, (SLAB, HEAD_DIM))
                else:
                    old = max_in[g, here]
                    top = jnp.maximum(old, jnp.max(scores, axis=1, keepdims=True))
                    shrink_ref[slot, here] = jnp.exp2(old - top)
                if not last:
                    max_out[g, here] = top
                parts = [
                    jnp.exp2(scores[:, b * rows:(b + 1) * rows] - top).astype(jnp.bfloat16)
                    for b in range(count)
                ]
                weights.append(jnp.concatenate(parts, axis=1))
            mixed = jnp.dot(
                jnp.concatenate(weights, axis=0),
                jnp.concatenate([v, ones], axis=1),
                preferred_element_type=jnp.float32,
            )
            for at in range(0, tall, SLAB):
                here = slice(at, at + SLAB)
                acc, total = mixed[here, :HEAD_DIM], mixed[here, HEAD_DIM:]
                if not first:
                    shrink = shrink_ref[slot, here]
                    acc = acc_in[g, here] * shrink + acc
                    total = sum_in[g, here] * shrink + total
                if last:
                    write(g, at, acc, total)
                else:
                    acc_out[g, here] = acc
                    sum_out[g, here] = total
            if last:
                copies.append(send(g))
        for copy in copies:
            copy.wait()

    if first:
        body()
        return
    me = lax.axis_index("seq")
    wanted = jnp.bool_(False)
    for i in users:
        wanted |= me == i
    pl.when(wanted)(body)

    @pl.when(jnp.logical_not(wanted))
    def _():
        if last:
            finish(lambda g, here: (acc_in[g, here], sum_in[g, here]))
        else:
            max_out[...] = max_in[...]
            sum_out[...] = sum_in[...]
            acc_out[...] = acc_in[...]


def attend(pieces, docs, places, q, mask, state=None, last=False):
    first = state is None
    count = len(places)
    rows = q.shape[1] // GROUP
    stacked = (KV_HEADS, GROUP * rows, HEAD_DIM)
    vmem = pl.BlockSpec(memory_space=pltpu.VMEM)
    args = [q, mask] + pieces + ([] if first else list(state))
    if last:
        out_shape = [jax.ShapeDtypeStruct((rows, HEADS * HEAD_DIM), jnp.bfloat16)]
    else:
        out_shape = [jax.ShapeDtypeStruct(stacked, jnp.float32)] * 3
    scratch = [
        pltpu.VMEM((2, GROUP * rows, count * rows), jnp.float32),
        pltpu.VMEM((2, GROUP * rows, HEAD_DIM), jnp.float32),
    ]
    if last:
        scratch += [pltpu.VMEM((rows, HEADS * HEAD_DIM), jnp.bfloat16), pltpu.SemaphoreType.DMA((KV_HEADS,))]
    users = [i for i in range(len(places[0])) if any(bases[i] != NOWHERE for bases in places)]
    return pl.pallas_call(
        functools.partial(attend_kernel, count, len(pieces), docs, first, last, users),
        out_shape=out_shape,
        in_specs=[vmem] * len(args),
        out_specs=[pl.BlockSpec(memory_space=pltpu.HBM)] if last else [vmem] * len(out_shape),
        scratch_shapes=scratch,
        cost_estimate=pl.CostEstimate(
            flops=4 * rows * HEADS * count * rows * HEAD_DIM,
            bytes_accessed=4 * 10**6,
            transcendentals=rows * HEADS * count * rows,
        ),
        compiler_params=pltpu.CompilerParams(vmem_limit_bytes=VMEM_LIMIT),
    )(*args)


def join_kernel(a_ref, b_ref, out_ref):
    rows = a_ref.shape[0]
    out_ref[:rows, :] = a_ref[...]
    out_ref[rows:, :] = b_ref[...]


def join(a, b):
    if a is None:
        return None
    vmem = pl.BlockSpec(memory_space=pltpu.VMEM)
    return pl.pallas_call(
        join_kernel,
        out_shape=jax.ShapeDtypeStruct((2 * a.shape[0], a.shape[1]), a.dtype),
        in_specs=[vmem] * 2,
        out_specs=vmem,
        cost_estimate=pl.CostEstimate(flops=10**5, bytes_accessed=10**6, transcendentals=0),
        compiler_params=pltpu.CompilerParams(vmem_limit_bytes=VMEM_LIMIT),
        name="join",
    )(a, b)


def block_reach(count):
    return -(-5 * count // 8)


def chip_reach_of(count):
    return -(-block_reach(count) // 2)


def per_device(count, queries, keys, values, doc_lengths):
    rows = queries.shape[0]
    reach, chip_reach = block_reach(count), chip_reach_of(count)

    seen = [set() for _ in range(count)]
    places = {}

    def place(name, pieces, last=False):
        table = []
        for piece in pieces:
            for b in range(len(piece.source[0])):
                bases = [NOWHERE] * count
                for i in range(count):
                    j = piece.source[i][b]
                    if i - reach <= j <= i and j not in seen[i]:
                        seen[i].add(j)
                        bases[i] = j * rows
                table.append(bases)
        places[name] = table

    source = [(i,) for i in range(count)]
    relay(Held(None, source), chip_reach, place)
    for i in range(count):
        assert seen[i] == set(range(max(0, i - reach), i + 1))

    own, cosine, sine = prepare(doc_lengths, keys, values)
    q, *masks = turn_queries(doc_lengths, queries, cosine, sine, list(places.values()))
    masks = dict(zip(places, masks))
    docs = doc_lengths.shape[0]
    held = {"state": None}

    def kernel(name, pieces, last=False):
        data = [p.data for p in pieces]
        held["state"] = attend(data, docs, places[name], q, masks[name], held["state"], last)

    relay(Held(own, source), chip_reach, kernel)
    return held["state"][0]


def solution(mesh):
    count = mesh.shape["seq"]

    def body(*args):
        return per_device(count, *args)

    return jax.shard_map(
        body,
        mesh=mesh,
        in_specs=(
            P(("grp", "seq"), None),
            P(("grp", "seq"), None),
            P(("grp", "seq"), None),
            P("grp"),
        ),
        out_specs=P(("grp", "seq"), None),
        check_vma=False,
    )
```

```python
import functools

import jax
import jax.numpy as jnp
from jax import lax
from jax.experimental import pallas as pl
from jax.experimental.pallas import tpu as pltpu
from jax.sharding import PartitionSpec as P


HEADS = 28
KV_HEADS = 4
HEAD_DIM = 128
GROUP = HEADS // KV_HEADS
ROPE_BASE = 1000000.0
SCORE_SCALE = HEAD_DIM ** (-0.5) * 1.4426950408889634
MASKED = -16384.0
NOWHERE = 1 << 28
VMEM_LIMIT = 24 * 1024 * 1024
SLAB = 32


class Held:
    def __init__(self, data, source):
        self.data, self.source = data, source

    def move(self, pairs):
        source = list(self.source)
        for s, t in pairs:
            source[t] = self.source[s]
        return Held(self.data if self.data is None else lax.ppermute(self.data, "seq", pairs), source)


def joined(a, b):
    return Held(join(a.data, b.data), [x + y for x, y in zip(a.source, b.source)])


def relay(own, chip_reach, kernel):
    count = len(own.source)

    def around(shift, first, narrow=False, via=False):
        span = count - first
        pairs = {}
        for i in range(count):
            if i < first or (narrow and i & 2):
                pairs[i] = i ^ 1
            else:
                pairs[i] = first + (i - first + shift) % span
        if via:
            for core in range(2):
                last, middle = count - shift + core, first - 2 + core
                pairs[last], pairs[middle] = middle, first + core
        assert sorted(pairs.values()) == list(range(count))
        return sorted(pairs.items())

    sibling = [(i, i ^ 1) for i in range(count)]
    across = [(i, i ^ 2) for i in range(count)]

    def swapped(pieces):
        both = pieces[0] if len(pieces) == 1 else joined(*pieces)
        return both.move(sibling)

    full, odd = chip_reach // 2, chip_reach % 2
    a = own
    for s in range(1, full + 1):
        b = a.move(across)
        here = a.move(around(4, 4 * (s - 1)))
        if s == 1:
            kernel("k0", [own, own.move(sibling)])
        kernel("k%d" % s, [here, b])
        kernel("kd%d" % s, [swapped([here, b])])
        a = here
    stage = full + 1
    if odd:
        c = b.move(around(4, 4 * (full - 1), True))
        pieces = [a.move(around(2, 4 * full)), c]
    else:
        pieces = [a.move(across)]
    kernel("k%d" % stage, pieces)
    kernel("last", [swapped(pieces)], True)


def rotated(x, cosine, sine):
    return x * cosine + pltpu.roll(x, HEAD_DIM // 2, 1) * sine


def in_hbm(x):
    return pltpu.with_memory_space_constraint(x, pltpu.HBM)


def lanes_iota(shape, dim):
    return lax.broadcasted_iota(jnp.int32, shape, dim)


def doc_starts(place, lengths_ref):
    start = jnp.zeros_like(place)
    end = 0
    for d in range(lengths_ref.shape[0]):
        end = end + lengths_ref[d]
        start = start + jnp.where(place >= end, lengths_ref[d], 0)
    return start


def prepare_kernel(freq_ref, lengths_hbm, k_hbm, v_hbm, kv_ref, cos_ref, sin_ref, lengths_ref, k_ref, sems):
    rows = k_ref.shape[0]
    width = KV_HEADS * HEAD_DIM
    copies = [
        pltpu.make_async_copy(lengths_hbm, lengths_ref, sems.at[0]),
        pltpu.make_async_copy(k_hbm, k_ref, sems.at[1]),
        pltpu.make_async_copy(v_hbm, kv_ref.at[:, pl.ds(width, width)], sems.at[2]),
    ]
    for copy in copies:
        copy.start()
    copies[0].wait()
    shape = (rows, HEAD_DIM)
    place = lax.axis_index("seq") * rows + lanes_iota(shape, 0)
    within = (place - doc_starts(place, lengths_ref)).astype(jnp.float32)
    angle = within * freq_ref[...]
    cosine = jnp.cos(angle)
    sine = jnp.sin(angle)
    sine = jnp.where(lanes_iota(shape, 1) < HEAD_DIM // 2, -sine, sine)
    cos_ref[...] = cosine
    sin_ref[...] = sine
    copies[1].wait()
    for g in range(KV_HEADS):
        cols = slice(g * HEAD_DIM, (g + 1) * HEAD_DIM)
        kv_ref[:, cols] = rotated(k_ref[:, cols].astype(jnp.float32), cosine, sine).astype(jnp.bfloat16)
    copies[2].wait()


def prepare(lengths, keys, values):
    rows = keys.shape[0]
    half = HEAD_DIM // 2
    lane = jnp.arange(HEAD_DIM, dtype=jnp.int32)[None, :]
    step = jnp.where(lane < half, lane, lane - half).astype(jnp.float32)
    freq = jnp.power(jnp.float32(ROPE_BASE), -2.0 * step / HEAD_DIM)
    vmem = pl.BlockSpec(memory_space=pltpu.VMEM)
    hbm = pl.BlockSpec(memory_space=pltpu.HBM)
    turn = jax.ShapeDtypeStruct((rows, HEAD_DIM), jnp.float32)
    return pl.pallas_call(
        prepare_kernel,
        out_shape=[jax.ShapeDtypeStruct((rows, 2 * KV_HEADS * HEAD_DIM), jnp.bfloat16), turn, turn],
        in_specs=[vmem, hbm, hbm, hbm],
        out_specs=[vmem] * 3,
        scratch_shapes=[
            pltpu.SMEM(lengths.shape, jnp.int32),
            pltpu.VMEM(keys.shape, keys.dtype),
            pltpu.SemaphoreType.DMA((3,)),
        ],
        cost_estimate=pl.CostEstimate(flops=10**6, bytes_accessed=6 * 10**5, transcendentals=0),
        compiler_params=pltpu.CompilerParams(vmem_limit_bytes=VMEM_LIMIT),
        name="prepare",
    )(freq, in_hbm(lengths), in_hbm(keys), in_hbm(values))


def turn_kernel(places, docs, lengths_hbm, q_hbm, cos_ref, sin_ref, *refs):
    q_ref, *rest = refs
    mask_refs, (lengths_ref, q_raw, sems) = rest[:-3], rest[-3:]
    rows = q_raw.shape[0]
    copies = [
        pltpu.make_async_copy(lengths_hbm, lengths_ref, sems.at[0]),
        pltpu.make_async_copy(q_hbm, q_raw, sems.at[1]),
    ]
    for copy in copies:
        copy.start()
    copies[0].wait()
    me = lax.axis_index("seq")
    square = (rows, HEAD_DIM)
    row, lane = lanes_iota(square, 0), lanes_iota(square, 1)
    first = jnp.full((8, HEAD_DIM), NOWHERE, jnp.int32)
    after = first
    end = 0
    for d in range(docs):
        here = lanes_iota((8, HEAD_DIM), 1) == d
        first = jnp.where(here, end, first)
        end = end + lengths_ref[d]
        after = jnp.where(here, end, after)
    first = jnp.broadcast_to(first[:1], square)
    after = jnp.broadcast_to(after[:1], square)
    for n, stage in enumerate(places):
        for b, bases in enumerate(stage):
            place = block_base(bases, me) + row
            member = (place >= first) & (place < after)
            mask_refs[n][b * rows:(b + 1) * rows, :] = jnp.where(member, 0.0, MASKED).astype(jnp.bfloat16)
    place = me * rows + row
    own_doc = jnp.where((place >= first) & (place < after), 1.0, 0.0)
    copies[1].wait()
    cosine, sine = cos_ref[...], sin_ref[...]
    for h in range(HEADS):
        head = q_raw[:, h * HEAD_DIM:(h + 1) * HEAD_DIM].astype(jnp.float32)
        g, at = h // GROUP, h % GROUP * rows
        turned = rotated(head, cosine, sine).astype(jnp.bfloat16).astype(jnp.float32) * SCORE_SCALE
        coarse = turned.astype(jnp.bfloat16)
        fine = turned - coarse.astype(jnp.float32)
        q_ref[g, at:at + rows, :HEAD_DIM] = coarse
        q_ref[g, at:at + rows, HEAD_DIM:] = jnp.where(lane < docs, own_doc, fine).astype(jnp.bfloat16)


def block_base(bases, me):
    base = jnp.int32(NOWHERE)
    for i, value in enumerate(bases):
        if value != NOWHERE:
            base = jnp.where(me == i, value, base)
    return base


def turn_queries(lengths, queries, cosine, sine, places):
    rows = queries.shape[0]
    assert rows == HEAD_DIM
    vmem = pl.BlockSpec(memory_space=pltpu.VMEM)
    hbm = pl.BlockSpec(memory_space=pltpu.HBM)
    out_shape = [jax.ShapeDtypeStruct((KV_HEADS, GROUP * rows, 2 * HEAD_DIM), jnp.bfloat16)]
    out_shape += [jax.ShapeDtypeStruct((len(stage) * rows, HEAD_DIM), jnp.bfloat16) for stage in places]
    return pl.pallas_call(
        functools.partial(turn_kernel, places, lengths.shape[0]),
        out_shape=out_shape,
        in_specs=[hbm, hbm, vmem, vmem],
        out_specs=[vmem] * len(out_shape),
        scratch_shapes=[
            pltpu.SMEM(lengths.shape, jnp.int32),
            pltpu.VMEM(queries.shape, queries.dtype),
            pltpu.SemaphoreType.DMA((2,)),
        ],
        cost_estimate=pl.CostEstimate(flops=10**8, bytes_accessed=4 * 10**6, transcendentals=0),
        compiler_params=pltpu.CompilerParams(vmem_limit_bytes=VMEM_LIMIT),
        name="turn_queries",
    )(in_hbm(lengths), in_hbm(queries), cosine, sine)


def attend_kernel(count, operands, docs, first, last, users, early, devices, *refs):
    refs = list(refs)
    take = lambda n: [refs.pop(0) for _ in range(n)]
    q_ref, mask_ref = take(2)
    kv_refs = take(operands)
    if not first:
        max_in, sum_in, acc_in = take(3)
    if last:
        take(1)
        (out_hbm,) = take(1)
    else:
        max_out, sum_out, acc_out = take(3)
        if early:
            (out_hbm,) = take(1)
    score_ref, shrink_ref = take(2)
    if last or early:
        out_ref, sems = take(2)

    rows = score_ref.shape[2] // count
    kv_refs = [r.at[n:n + rows] for r in kv_refs for n in range(0, r.shape[0], rows)]
    width = KV_HEADS * HEAD_DIM
    tall = GROUP * rows
    key_lane = lanes_iota((count * rows, HEAD_DIM), 1)
    ones = jnp.ones((count * rows, HEAD_DIM), jnp.bfloat16)

    def write(g, at, acc, total):
        head, row = g * GROUP + at // rows, at % rows
        cols = slice(head * HEAD_DIM, (head + 1) * HEAD_DIM)
        out_ref[row:row + SLAB, cols] = (acc / total).astype(jnp.bfloat16)

    def send(g):
        cols = pl.ds(g * GROUP * HEAD_DIM, GROUP * HEAD_DIM)
        copy = pltpu.make_async_copy(out_ref.at[:, cols], out_hbm.at[:, cols], sems.at[g])
        copy.start()
        return copy

    def finish(result):
        copies = []
        for g in range(KV_HEADS):
            for at in range(0, tall, SLAB):
                write(g, at, *result(g, slice(at, at + SLAB)))
            copies.append(send(g))
        for copy in copies:
            copy.wait()

    def body():
        def score(g):
            k = jnp.concatenate([r[:, g * HEAD_DIM:(g + 1) * HEAD_DIM] for r in kv_refs], axis=0)
            k = jnp.concatenate([k, jnp.where(key_lane < docs, mask_ref[...], k)], axis=1)
            return lax.dot_general(q_ref[g], k, (((1,), (1,)), ((), ())), preferred_element_type=jnp.float32)

        copies = []
        score_ref[0] = score(0)
        for g in range(KV_HEADS):
            slot = g % 2
            if g + 1 < KV_HEADS:
                score_ref[1 - slot] = score(g + 1)
            v = jnp.concatenate(
                [r[:, width + g * HEAD_DIM:width + (g + 1) * HEAD_DIM] for r in kv_refs], axis=0
            )
            weights = []
            for at in range(0, tall, SLAB):
                here = slice(at, at + SLAB)
                scores = score_ref[slot, here]
                if first:
                    shape = (SLAB, count * rows)
                    after = lanes_iota(shape, 1) - lanes_iota(shape, 0) > at % rows
                    after &= lanes_iota(shape, 1) < rows
                    scores = jnp.where(after, MASKED, scores)
                    top = jnp.max(scores, axis=1, keepdims=True)
                    top = jnp.broadcast_to(top, (SLAB, HEAD_DIM))
                else:
                    old = max_in[g, here]
                    top = jnp.maximum(old, jnp.max(scores, axis=1, keepdims=True))
                    shrink_ref[slot, here] = jnp.exp2(old - top)
                if not last:
                    max_out[g, here] = top
                parts = [
                    jnp.exp2(scores[:, b * rows:(b + 1) * rows] - top).astype(jnp.bfloat16)
                    for b in range(count)
                ]
                weights.append(jnp.concatenate(parts, axis=1))
            mixed = jnp.dot(
                jnp.concatenate(weights, axis=0),
                jnp.concatenate([v, ones], axis=1),
                preferred_element_type=jnp.float32,
            )
            for at in range(0, tall, SLAB):
                here = slice(at, at + SLAB)
                acc, total = mixed[here, :HEAD_DIM], mixed[here, HEAD_DIM:]
                if not first:
                    shrink = shrink_ref[slot, here]
                    acc = acc_in[g, here] * shrink + acc
                    total = sum_in[g, here] * shrink + total
                if last:
                    write(g, at, acc, total)
                else:
                    acc_out[g, here] = acc
                    sum_out[g, here] = total
            if last:
                copies.append(send(g))
        for copy in copies:
            copy.wait()

    if first:
        body()
        return
    me = lax.axis_index("seq")

    def among(devices):
        found = jnp.bool_(False)
        for i in devices:
            found |= me == i
        return found

    pl.when(among(users))(body)
    if not last:

        @pl.when(among([i for i in range(devices) if i not in users and i not in early]))
        def _():
            max_out[...] = max_in[...]
            sum_out[...] = sum_in[...]
            acc_out[...] = acc_in[...]

    if last or early:
        ending = [i for i in range(devices) if i not in users and i not in early] if last else early

        @pl.when(among(ending))
        def _():
            finish(lambda g, here: (acc_in[g, here], sum_in[g, here]))


def users_of(places):
    return [i for i in range(len(places[0])) if any(bases[i] != NOWHERE for bases in places)]


def attend(pieces, docs, places, q, mask, state=None, last=False, early=()):
    first = state is None
    count = len(places)
    rows = q.shape[1] // GROUP
    stacked = (KV_HEADS, GROUP * rows, HEAD_DIM)
    vmem = pl.BlockSpec(memory_space=pltpu.VMEM)
    args = [q, mask] + pieces + ([] if first else list(state))
    result = jax.ShapeDtypeStruct((rows, HEADS * HEAD_DIM), jnp.bfloat16)
    if last:
        out_shape = [result]
    else:
        out_shape = [jax.ShapeDtypeStruct(stacked, jnp.float32)] * 3 + ([result] if early else [])
    scratch = [
        pltpu.VMEM((2, GROUP * rows, count * rows), jnp.float32),
        pltpu.VMEM((2, GROUP * rows, HEAD_DIM), jnp.float32),
    ]
    if last or early:
        scratch += [pltpu.VMEM((rows, HEADS * HEAD_DIM), jnp.bfloat16), pltpu.SemaphoreType.DMA((KV_HEADS,))]
    hbm = pl.BlockSpec(memory_space=pltpu.HBM)
    users = users_of(places)
    return pl.pallas_call(
        functools.partial(attend_kernel, count, len(pieces), docs, first, last, users, early, len(places[0])),
        out_shape=out_shape,
        in_specs=[hbm if last and n == len(args) - 1 else vmem for n in range(len(args))],
        out_specs=[hbm if x is result else vmem for x in out_shape],
        input_output_aliases={len(args) - 1: 0} if last else {},
        scratch_shapes=scratch,
        cost_estimate=pl.CostEstimate(
            flops=4 * rows * HEADS * count * rows * HEAD_DIM,
            bytes_accessed=4 * 10**6,
            transcendentals=rows * HEADS * count * rows,
        ),
        compiler_params=pltpu.CompilerParams(vmem_limit_bytes=VMEM_LIMIT),
    )(*args)


def join_kernel(a_ref, b_ref, out_ref):
    rows = a_ref.shape[0]
    out_ref[:rows, :] = a_ref[...]
    out_ref[rows:, :] = b_ref[...]


def join(a, b):
    if a is None:
        return None
    vmem = pl.BlockSpec(memory_space=pltpu.VMEM)
    return pl.pallas_call(
        join_kernel,
        out_shape=jax.ShapeDtypeStruct((2 * a.shape[0], a.shape[1]), a.dtype),
        in_specs=[vmem] * 2,
        out_specs=vmem,
        cost_estimate=pl.CostEstimate(flops=10**5, bytes_accessed=10**6, transcendentals=0),
        compiler_params=pltpu.CompilerParams(vmem_limit_bytes=VMEM_LIMIT),
        name="join",
    )(a, b)


def block_reach(count):
    return -(-5 * count // 8)


def chip_reach_of(count):
    return -(-block_reach(count) // 2)


def per_device(count, queries, keys, values, doc_lengths):
    rows = queries.shape[0]
    reach, chip_reach = block_reach(count), chip_reach_of(count)

    seen = [set() for _ in range(count)]
    places = {}

    def place(name, pieces, last=False):
        table = []
        for piece in pieces:
            for b in range(len(piece.source[0])):
                bases = [NOWHERE] * count
                for i in range(count):
                    j = piece.source[i][b]
                    if i - reach <= j <= i and j not in seen[i]:
                        seen[i].add(j)
                        bases[i] = j * rows
                table.append(bases)
        places[name] = table

    source = [(i,) for i in range(count)]
    relay(Held(None, source), chip_reach, place)
    for i in range(count):
        assert seen[i] == set(range(max(0, i - reach), i + 1))

    own, cosine, sine = prepare(doc_lengths, keys, values)
    q, *masks = turn_queries(doc_lengths, queries, cosine, sine, list(places.values()))
    masks = dict(zip(places, masks))
    docs = doc_lengths.shape[0]
    held = {"state": None}
    before_last = list(places)[-2]
    busy = users_of(places[before_last]) + users_of(places["last"])
    early = [i for i in range(count) if i not in busy]

    def kernel(name, pieces, last=False):
        data = [p.data for p in pieces]
        ends = early if last or name == before_last else ()
        held["state"] = attend(data, docs, places[name], q, masks[name], held["state"], last, ends)

    relay(Held(own, source), chip_reach, kernel)
    return held["state"][0]


def solution(mesh):
    count = mesh.shape["seq"]

    def body(*args):
        return per_device(count, *args)

    return jax.shard_map(
        body,
        mesh=mesh,
        in_specs=(
            P(("grp", "seq"), None),
            P(("grp", "seq"), None),
            P(("grp", "seq"), None),
            P("grp"),
        ),
        out_specs=P(("grp", "seq"), None),
        check_vma=False,
    )
```
